16 devices in a mesh: rep: 2 (over z), fsdp: 8 (over y, x, core).
Axes of the slice: x: 2, y: 2, z: 2, core: 2. Of those that a mesh axis runs over, the one named last changes fastest.
Arguments:
- x_tokens: bfloat16 [512, 50, 1024], P(('rep', 'fsdp'))
- grad_z: bfloat16 [512, 50, 1024], P(('rep', 'fsdp'))
- w_qkv: float32 [1024, 3072], P('fsdp')
- b_qkv: float32 [3072], P('fsdp')
- w_out: float32 [1024, 1024], P('fsdp')
- w_up: float32 [1024, 4096], P('fsdp')
- b_up: float32 [4096], P('fsdp')
- w_down: float32 [4096, 1024], P('fsdp')
- vec_params: float32 [8, 1024], P(None, 'fsdp')
Outputs:
- output 1: bfloat16 [512, 50, 1024], P(('rep', 'fsdp'))
- output 2: bfloat16 [512, 50, 1024], P(('rep', 'fsdp'))
- output 3: float32 [1024, 3072], P('fsdp')
- output 4: float32 [3072], P('fsdp')
- output 5: float32 [1024, 1024], P('fsdp')
- output 6: float32 [1024, 4096], P('fsdp')
- output 7: float32 [4096], P('fsdp')
- output 8: float32 [4096, 1024], P('fsdp')
- output 9: float32 [8, 1024], P(None, 'fsdp')
All inputs are finite; a program needn't handle non-finite values.
Results may differ from the reference program's by a relative error of at most 0.02.
Values are sent between devices in bfloat16 or wider.
A program may use at most 1 GiB of HBM per device.

```python
import jax
import jax.numpy as jnp
from jax import lax

D = 1024
FF = 4096
SEQ = 50
HEADS = 16
SEQS_DEV = 32
DEVICES = 16
BATCH = SEQS_DEV * DEVICES
HEAD = D // HEADS
LN_EPS = 1e-5


def setup_inputs(seed: int = 0) -> dict:
    keys = jax.random.split(jax.random.key(seed), 12)
    seq_scale = jax.random.uniform(keys[0], (BATCH, 1, 1), minval=0.5, maxval=2.0)
    x_tokens = (jax.random.normal(keys[1], (BATCH, SEQ, D)) * seq_scale).astype(jnp.bfloat16)
    grad_scale = jax.random.uniform(keys[2], (BATCH, 1, 1), minval=0.25, maxval=2.0)
    grad_z = (jax.random.normal(keys[3], (BATCH, SEQ, D)) * grad_scale).astype(jnp.bfloat16)
    w_qkv = jax.random.normal(keys[4], (D, 3 * D)) * D ** -0.5
    b_qkv = 0.5 * jax.random.normal(keys[5], (3 * D,))
    w_out = jax.random.normal(keys[6], (D, D)) * D ** -0.5
    w_up = jax.random.normal(keys[7], (D, FF)) * D ** -0.5
    b_up = 0.5 * jax.random.normal(keys[8], (FF,))
    w_down = jax.random.normal(keys[9], (FF, D)) * FF ** -0.5
    is_scale = jnp.array([0.0, 0.0, 0.0, 1.0, 0.0, 0.0, 0.0, 1.0], jnp.float32)[:, None]
    row_offset = jnp.array([1.0, 0.0, 0.0, 0.0, 1.0, 0.0, 0.0, 0.0], jnp.float32)[:, None]
    normal_rows = row_offset + 0.25 * jax.random.normal(keys[10], (8, D))
    scale_rows = jax.random.uniform(keys[11], (8, D), minval=0.5, maxval=1.5)
    vec_params = is_scale * scale_rows + (1.0 - is_scale) * normal_rows
    return {"x_tokens": x_tokens, "grad_z": grad_z, "w_qkv": w_qkv, "b_qkv": b_qkv, "w_out": w_out,
            "w_up": w_up, "b_up": b_up, "w_down": w_down, "vec_params": vec_params}


def normalize(t):
    mean = jnp.mean(t, axis=-1, keepdims=True)
    centered = t - mean
    variance = jnp.mean(centered * centered, axis=-1, keepdims=True)
    return centered * lax.rsqrt(variance + LN_EPS)


def gelu_exact(t):
    return jax.nn.gelu(t, approximate=False)


def layer_pass(x_seq, dz_seq, matrices, bias_qkv, bias_up, vec_rows):
    w_qkv, w_out, w_up, w_down = matrices
    ln1_gain, ln1_bias, out_bias, scale_attn, ln2_gain, ln2_bias, down_bias, scale_mlp = vec_rows
    score_scale = HEAD ** -0.5
    x_float = x_seq.astype(jnp.float32)
    xhat_one, norm_one_back = jax.vjp(normalize, x_float)
    h_one = (xhat_one * ln1_gain + ln1_bias).astype(jnp.bfloat16)
    qkv_proj = (jnp.dot(h_one, w_qkv, preferred_element_type=jnp.float32) + bias_qkv).astype(jnp.bfloat16)
    qkv_heads = qkv_proj.reshape(SEQ, 3, HEADS, HEAD).astype(jnp.float32)
    q_heads = qkv_heads[:, 0]
    k_heads = qkv_heads[:, 1]
    v_heads = qkv_heads[:, 2]
    scores = jnp.einsum("qhe,khe->hqk", q_heads, k_heads) * score_scale
    attn_probs = jax.nn.softmax(scores, axis=-1)
    probs_bf = attn_probs.astype(jnp.bfloat16).astype(jnp.float32)
    head_out = jnp.einsum("hqk,khe->qhe", probs_bf, v_heads).astype(jnp.bfloat16).reshape(SEQ, D)
    att_out = jnp.dot(head_out, w_out, preferred_element_type=jnp.float32) + out_bias
    resid_mid = x_float + scale_attn * att_out
    xhat_two, norm_two_back = jax.vjp(normalize, resid_mid)
    h_two = (xhat_two * ln2_gain + ln2_bias).astype(jnp.bfloat16)
    pre_act = jnp.dot(h_two, w_up, preferred_element_type=jnp.float32) + bias_up
    act_float, gelu_back = jax.vjp(gelu_exact, pre_act)
    mlp_act = act_float.astype(jnp.bfloat16)
    mlp_out = jnp.dot(mlp_act, w_down, preferred_element_type=jnp.float32) + down_bias
    z_seq = (resid_mid + scale_mlp * mlp_out).astype(jnp.bfloat16)
    g_out = dz_seq.astype(jnp.float32)
    grad_scale_mlp = jnp.sum(g_out * mlp_out, axis=0)
    d_mlp = g_out * scale_mlp
    grad_down_bias = jnp.sum(d_mlp, axis=0)
    d_mlp_bf = d_mlp.astype(jnp.bfloat16)
    grad_w_down = jnp.dot(mlp_act.T, d_mlp_bf, preferred_element_type=jnp.float32)
    d_act = jnp.dot(d_mlp_bf, w_down.T, preferred_element_type=jnp.float32)
    d_pre = gelu_back(d_act)[0]
    grad_b_up = jnp.sum(d_pre, axis=0)
    d_pre_bf = d_pre.astype(jnp.bfloat16)
    grad_w_up = jnp.dot(h_two.T, d_pre_bf, preferred_element_type=jnp.float32)
    d_h_two = jnp.dot(d_pre_bf, w_up.T, preferred_element_type=jnp.float32)
    grad_ln2_gain = jnp.sum(d_h_two * xhat_two, axis=0)
    grad_ln2_bias = jnp.sum(d_h_two, axis=0)
    g_resid = g_out + norm_two_back(d_h_two * ln2_gain)[0]
    grad_scale_attn = jnp.sum(g_resid * att_out, axis=0)
    d_att = g_resid * scale_attn
    grad_out_bias = jnp.sum(d_att, axis=0)
    d_att_bf = d_att.astype(jnp.bfloat16)
    grad_w_out = jnp.dot(head_out.T, d_att_bf, preferred_element_type=jnp.float32)
    d_heads = jnp.dot(d_att_bf, w_out.T, preferred_element_type=jnp.float32).astype(jnp.bfloat16)
    d_heads = d_heads.reshape(SEQ, HEADS, HEAD).astype(jnp.float32)
    d_probs = jnp.einsum("qhe,khe->hqk", d_heads, v_heads)
    grad_v = jnp.einsum("hqk,qhe->khe", probs_bf, d_heads)
    d_scores = attn_probs * (d_probs - jnp.sum(d_probs * attn_probs, axis=-1, keepdims=True))
    d_scores_bf = (d_scores * score_scale).astype(jnp.bfloat16).astype(jnp.float32)
    grad_q = jnp.einsum("hqk,khe->qhe", d_scores_bf, k_heads)
    grad_k = jnp.einsum("hqk,qhe->khe", d_scores_bf, q_heads)
    d_qkv = jnp.stack([grad_q, grad_k, grad_v], axis=1).reshape(SEQ, 3 * D)
    grad_b_qkv = jnp.sum(d_qkv, axis=0)
    d_qkv_bf = d_qkv.astype(jnp.bfloat16)
    grad_w_qkv = jnp.dot(h_one.T, d_qkv_bf, preferred_element_type=jnp.float32)
    d_h_one = jnp.dot(d_qkv_bf, w_qkv.T, preferred_element_type=jnp.float32)
    grad_ln1_gain = jnp.sum(d_h_one * xhat_one, axis=0)
    grad_ln1_bias = jnp.sum(d_h_one, axis=0)
    dx_seq = (g_resid + norm_one_back(d_h_one * ln1_gain)[0]).astype(jnp.bfloat16)
    grad_vec = jnp.stack([grad_ln1_gain, grad_ln1_bias, grad_out_bias, grad_scale_attn,
                          grad_ln2_gain, grad_ln2_bias, grad_down_bias, grad_scale_mlp])
    return z_seq, dx_seq, (grad_w_qkv, grad_b_qkv, grad_w_out, grad_w_up, grad_b_up, grad_w_down, grad_vec)


def reference(x_tokens, grad_z, w_qkv, b_qkv, w_out, w_up, b_up, w_down, vec_params):
    matrices = (w_qkv.astype(jnp.bfloat16), w_out.astype(jnp.bfloat16),
                w_up.astype(jnp.bfloat16), w_down.astype(jnp.bfloat16))
    bias_qkv = b_qkv.astype(jnp.bfloat16).astype(jnp.float32)
    bias_up = b_up.astype(jnp.bfloat16).astype(jnp.float32)
    vec_rows = vec_params.astype(jnp.bfloat16).astype(jnp.float32)

    def step(running, pair):
        z_seq, dx_seq, seq_grads = layer_pass(pair[0], pair[1], matrices, bias_qkv, bias_up, vec_rows)
        return jax.tree.map(jnp.add, running, seq_grads), (z_seq, dx_seq)

    zero_grads = (jnp.zeros((D, 3 * D), jnp.float32), jnp.zeros((3 * D,), jnp.float32),
                  jnp.zeros((D, D), jnp.float32), jnp.zeros((D, FF), jnp.float32),
                  jnp.zeros((FF,), jnp.float32), jnp.zeros((FF, D), jnp.float32),
                  jnp.zeros((8, D), jnp.float32))
    totals, seq_outs = lax.scan(step, zero_grads, (x_tokens, grad_z))
    grad_w_qkv, grad_b_qkv, grad_w_out, grad_w_up, grad_b_up, grad_w_down, grad_vec = totals
    return (seq_outs[0], seq_outs[1], grad_w_qkv, grad_b_qkv, grad_w_out, grad_w_up, grad_b_up,
            grad_w_down, grad_vec)
```

```python
import functools

import jax
import jax.numpy as jnp
from jax import lax
from jax.experimental import pallas as pl
from jax.experimental.layout import Layout, with_layout_constraint
from jax.experimental.pallas import tpu as pltpu
from jax.sharding import PartitionSpec as P


HEADS = 16
LN_EPS = 1e-5
SEQ = 50
D = 1024
FF = 4096
SEQS = 32
T = SEQS * SEQ
NS = 8
CHUNKS = 2
HALF = D // 2
FC = FF // NS // CHUNKS
GROUP = 8
ROWS = GROUP * SEQ
PAIR = 2 * SEQ
WIN = 112
SCALE = (D // HEADS) ** -0.5
NEG = -3.0e38
F32 = jnp.float32
BF16 = jnp.bfloat16

ERFC_P = 0.45
ERFC_Q = (0.25388532876968384, 0.25388315320014954, 0.22827185690402985, 0.1752501279115677, 0.11996052414178848,
          -0.0223874319344759, 0.14245237410068512, -0.30063509941101074, 0.19071702659130096, -0.041397832334041595)


def dot(a, b):
    return lax.dot_general(a, b, (((1,), (0,)), ((), ())), preferred_element_type=F32)


def dot_nt(a, b):
    return lax.dot_general(a, b, (((1,), (1,)), ((), ())), preferred_element_type=F32)


def dot_tn(a, b):
    return lax.dot_general(a, b, (((0,), (0,)), ((), ())), preferred_element_type=F32)


def gelu_and_slope(u):
    dens = jnp.exp(u * u * -0.5)
    t = 1.0 / (1.0 + (ERFC_P * 0.5 ** 0.5) * jnp.abs(u))
    q = jnp.full_like(t, ERFC_Q[-1])
    for coef in ERFC_Q[-2::-1]:
        q = q * t + coef
    half = (0.5 * dens) * (t * q)
    cdf = jnp.where(u > 0, 1.0 - half, half)
    return u * cdf, cdf + u * dens * 0.3989422804014327


def window_parts(j):
    start = 16 * ((PAIR * j) // 16)
    off = PAIR * j - start
    r = lax.broadcasted_iota(jnp.int32, (WIN, WIN), 0)
    c = lax.broadcasted_iota(jnp.int32, (WIN, WIN), 1)

    def seq_of(v):
        one = jnp.int32(1)
        zero = jnp.int32(0)
        return (jnp.where(v >= off, one, zero) + jnp.where(v >= off + SEQ, one, zero)
                + jnp.where(v >= off + PAIR, one, zero))

    bias = jnp.where(seq_of(r) == seq_of(c), 0.0, NEG)
    row = lax.broadcasted_iota(jnp.int32, (WIN, 128), 0)
    lane = lax.broadcasted_iota(jnp.int32, (WIN, 128), 1)
    inside = (row >= off) & (row < off + PAIR)
    return start, bias, inside, lane < 64


def softmax_rows(s, bias2):
    s = jnp.where(bias2 == 0.0, s, NEG)
    m = jnp.max(s, axis=1, keepdims=True)
    p = jnp.exp((s - m) * SCALE)
    return p * (1.0 / jnp.sum(p, axis=1, keepdims=True))


def attn_fwd_kernel(q_ref, k_ref, v_ref, o_ref):
    for j in range(ROWS // PAIR):
        start, bias, inside, even = window_parts(j)
        bias2 = jnp.concatenate([bias, bias], axis=0)
        m_even = jnp.where(even, 1.0, 0.0).astype(BF16)
        m_odd = jnp.where(even, 0.0, 1.0).astype(BF16)
        for hp in range(q_ref.shape[1] // 128):
            cols = slice(hp * 128, hp * 128 + 128)
            q = q_ref[start:start + WIN, cols]
            k = k_ref[start:start + WIN, cols]
            v = v_ref[start:start + WIN, cols]
            q2 = jnp.concatenate([q * m_even, q * m_odd], axis=0)
            p = softmax_rows(dot_nt(q2, k), bias2)
            o2 = dot(p.astype(BF16), v)
            o = jnp.where(inside, jnp.where(even, o2[:WIN], o2[WIN:]), 0.0).astype(BF16)
            if j:
                o_ref[start:start + 16, cols] += o[:16]
                o_ref[start + 16:start + WIN, cols] = o[16:]
            else:
                o_ref[start:start + WIN, cols] = o


def attn_bwd_kernel(q_ref, k_ref, v_ref, g_ref, d_ref, b_ref):
    parts = []
    for j in range(ROWS // PAIR):
        start, bias, inside, even = window_parts(j)
        one_even = jnp.where(even, 1.0, 0.0)
        parts.append((start, jnp.concatenate([bias, bias], axis=0), one_even.astype(BF16), (1.0 - one_even).astype(BF16),
                      jnp.where(inside, one_even, 0.0).astype(BF16), jnp.where(inside, 1.0 - one_even, 0.0).astype(BF16)))

    def head_pair(hp, carry):
        cols = pl.ds(pl.multiple_of(hp * 128, 128), 128)
        sums = [jnp.zeros((1, 128), F32) for _ in range(3)]
        for j, (start, bias2, m_even, m_odd, g_even, g_odd) in enumerate(parts):
            q = q_ref[start:start + WIN, cols]
            k = k_ref[start:start + WIN, cols]
            v = v_ref[start:start + WIN, cols]
            g = g_ref[start:start + WIN, cols]
            q2 = jnp.concatenate([q * m_even, q * m_odd], axis=0)
            g2 = jnp.concatenate([g * g_even, g * g_odd], axis=0)
            p = softmax_rows(dot_nt(q2, k), bias2)
            dp = dot_nt(g2, v)
            ds = (p * (dp - jnp.sum(dp * p, axis=1, keepdims=True)) * SCALE).astype(BF16)
            dq2 = dot(ds, k)
            even = lax.broadcasted_iota(jnp.int32, (WIN, 128), 1) < 64
            dq = jnp.where(even, dq2[:WIN], dq2[WIN:])
            dk = dot_tn(ds, q2)
            dv = dot_tn(p.astype(BF16), g2)
            for i, val in enumerate((dq, dk, dv)):
                out = pl.ds(pl.multiple_of(hp * 128 + i * HALF, 128), 128)
                sums[i] = sums[i] + jnp.sum(val, axis=0, keepdims=True)
                val = val.astype(BF16)
                if j:
                    d_ref[start:start + 16, out] += val[:16]
                    d_ref[start + 16:start + WIN, out] = val[16:]
                else:
                    d_ref[start:start + WIN, out] = val
        for i in range(3):
            b_ref[0, :, pl.ds(pl.multiple_of(hp * 128 + i * HALF, 128), 128)] = sums[i]
        return carry

    lax.fori_loop(0, HALF // 128, head_pair, 0)


ATT_COLS = 256


def attn_forward(qkv):
    per = HALF // ATT_COLS
    spec = lambda part: pl.BlockSpec((ROWS, ATT_COLS), lambda g, c: (g, (c // per * 3 + part) * per + c % per))
    return pl.pallas_call(
        attn_fwd_kernel,
        grid=(T // ROWS, D // ATT_COLS),
        in_specs=[spec(0), spec(1), spec(2)],
        out_specs=pl.BlockSpec((ROWS, ATT_COLS), lambda g, c: (g, c)),
        out_shape=jax.ShapeDtypeStruct((T, D), BF16),
        compiler_params=pltpu.CompilerParams(dimension_semantics=("arbitrary", "arbitrary")),
        cost_estimate=pl.CostEstimate(flops=8_000_000_000, bytes_accessed=13_000_000, transcendentals=3_000_000),
        name="attn_fwd",
    )(qkv, qkv, qkv)


def attn_backward(qkv, d_heads, half):
    spec = lambda at: pl.BlockSpec((ROWS, HALF), lambda g: (g, at))
    return pl.pallas_call(
        attn_bwd_kernel,
        grid=(T // ROWS,),
        in_specs=[spec(3 * half), spec(3 * half + 1), spec(3 * half + 2), spec(half)],
        out_specs=[pl.BlockSpec((ROWS, 3 * HALF), lambda g: (g, 0)), pl.BlockSpec((1, 1, 3 * HALF), lambda g: (g, 0, 0))],
        out_shape=[jax.ShapeDtypeStruct((T, 3 * HALF), BF16), jax.ShapeDtypeStruct((T // ROWS, 1, 3 * HALF), F32)],
        compiler_params=pltpu.CompilerParams(dimension_semantics=("arbitrary",)),
        cost_estimate=pl.CostEstimate(flops=16_000_000_000, bytes_accessed=12_000_000, transcendentals=1_500_000),
        name="attn_bwd",
    )(qkv, qkv, qkv, d_heads)


MLP_ROWS = 400
BLK = 2 * FC


def mlp_kernel(h_ref, g_ref, ht_ref, gt_ref, w1_ref, wd_ref, b1_ref, m_ref, dh_ref,
               gw1_send, gw1_keep, gw2_send, gw2_keep, gb_ref, act_s, dpre_s, w2_ref):
    step = pl.program_id(0)
    core = lax.rem(lax.axis_index("fsdp"), 2)
    gb_ref[...] = jnp.zeros_like(gb_ref)
    for n in range(4):
        w2_ref[n * 128:(n + 1) * 128, :] = wd_ref[n // 2, :, n % 2 * D:(n % 2 + 1) * D]

    @pl.when(step == 0)
    def _():
        m_ref[...] = jnp.zeros_like(m_ref)
        dh_ref[...] = jnp.zeros_like(dh_ref)

    def rows_step(i, carry):
        rows = pl.ds(pl.multiple_of(i * MLP_ROWS, 16), MLP_ROWS)
        w1 = w1_ref[...].reshape(D, BLK)
        u = dot(h_ref[rows, :], w1) + b1_ref[...]
        d_act = dot_nt(g_ref[rows, :], w2_ref[...])
        act, slope = gelu_and_slope(u)
        act = act.astype(BF16)
        d_pre = d_act * slope
        gb_ref[...] += jnp.sum(d_pre, axis=0, keepdims=True)
        d_pre = d_pre.astype(BF16)
        act_s[rows, :] = act
        dpre_s[rows, :] = d_pre
        m_ref[rows, :] += dot(act, w2_ref[...])
        dh_ref[rows, :] += dot_nt(d_pre, w1)
        return carry

    lax.fori_loop(0, T // MLP_ROWS, rows_step, 0)

    def grad_step(i, carry):
        for side, out in ((1 - core, gw1_send), (core, gw1_keep)):
            rows = pl.ds(pl.multiple_of((2 * i + side) * 128, 128), 128)
            out[i] = dot(ht_ref[rows, :], dpre_s[...])
        rows = pl.ds(pl.multiple_of(i * 256, 256), 256)
        for side, out in ((1 - core, gw2_send), (core, gw2_keep)):
            out[0, rows, :] = dot(gt_ref[rows, :], act_s[:, pl.ds(pl.multiple_of(side * FC, FC), FC)])
        return carry

    lax.fori_loop(0, D // 256, grad_step, 0)


def mlp_chunk(h, g, ht, gt, weights, b1):
    cols = NS * FC
    once = pl.Buffered(1)
    whole = lambda shape: pl.BlockSpec(shape, lambda s: (0, 0), pipeline_mode=once)
    return pl.pallas_call(
        mlp_kernel,
        grid=(cols // BLK,),
        in_specs=[whole((T, D)), whole((T, D)), whole((D, T)), whole((D, T)),
                  pl.BlockSpec((NS, D // NS, BLK), lambda s: (0, 0, s)),
                  pl.BlockSpec((2, D // NS, cols), lambda s: (s, 1, 0)),
                  pl.BlockSpec((1, BLK), lambda s: (0, s))],
        out_specs=[whole((T, D)), whole((T, D)),
                   *[pl.BlockSpec((4, D // NS, BLK), lambda s: (0, 0, s))] * 2,
                   *[pl.BlockSpec((1, D, FC), lambda s: (s, 0, 0))] * 2,
                   pl.BlockSpec((1, BLK), lambda s: (0, s))],
        out_shape=[jax.ShapeDtypeStruct((T, D), F32), jax.ShapeDtypeStruct((T, D), F32),
                   *[jax.ShapeDtypeStruct((4, D // NS, cols), F32)] * 2, *[jax.ShapeDtypeStruct((4, D, FC), F32)] * 2,
                   jax.ShapeDtypeStruct((1, cols), F32)],
        scratch_shapes=[pltpu.VMEM((T, BLK), BF16), pltpu.VMEM((T, BLK), BF16), pltpu.VMEM((BLK, D), BF16)],
        compiler_params=pltpu.CompilerParams(dimension_semantics=("arbitrary",), vmem_limit_bytes=62 * 1024 * 1024),
        cost_estimate=pl.CostEstimate(flops=12 * T * D * cols, bytes_accessed=60_000_000, transcendentals=T * cols),
        name="mlp_fwd_bwd",
    )(h, g, ht, gt, weights, weights, b1)


POST_ROWS = 200


def post_kernel(m0_ref, m1_ref, d0_ref, d1_ref, x_ref, att_ref, g_ref, vec_ref, z_ref, res_ref, da_ref, sum_ref):
    row = lambda i: vec_ref[i:i + 1, :]
    att = att_ref[...]
    y = x_ref[...].astype(F32) + row(3) * att
    m = m0_ref[...] + m1_ref[...] + row(6)
    g = g_ref[...].astype(F32)
    z_ref[...] = (y + row(7) * m).astype(BF16)
    xhat, rstd = ln_stats(y)
    dh = d0_ref[...] + d1_ref[...]
    res = g + ln_back(xhat, rstd, dh * row(4))
    res_ref[...] = res
    da = res * row(3)
    da_ref[...] = da.astype(BF16)

    @pl.when(pl.program_id(0) == 0)
    def _():
        sum_ref[...] = jnp.zeros_like(sum_ref)

    for i, val in ((2, da), (3, res * att), (4, dh * xhat), (5, dh), (6, g * row(7)), (7, g * m)):
        sum_ref[i:i + 1, :] += jnp.sum(val, axis=0, keepdims=True)


def post_mlp(m0, m1, d0, d1, x, att, g, vec):
    rows = pl.BlockSpec((POST_ROWS, D), lambda i: (i, 0))
    fixed = pl.BlockSpec((8, D), lambda i: (0, 0))
    return pl.pallas_call(
        post_kernel,
        grid=(T // POST_ROWS,),
        in_specs=[rows] * 7 + [fixed],
        out_specs=[rows, rows, rows, fixed],
        out_shape=[jax.ShapeDtypeStruct((T, D), BF16), jax.ShapeDtypeStruct((T, D), F32), jax.ShapeDtypeStruct((T, D), BF16),
                   jax.ShapeDtypeStruct((8, D), F32)],
        compiler_params=pltpu.CompilerParams(dimension_semantics=("arbitrary",)),
        cost_estimate=pl.CostEstimate(flops=5_000_000_000, bytes_accessed=56_000_000, transcendentals=T),
        name="post_mlp",
    )(m0, m1, d0, d1, x, att, g, vec)


def ln_stats(t):
    mean = jnp.mean(t, axis=-1, keepdims=True)
    centered = t - mean
    variance = jnp.mean(centered * centered, axis=-1, keepdims=True)
    rstd = lax.rsqrt(variance + LN_EPS)
    return centered * rstd, rstd


def ln_back(xhat, rstd, d):
    return rstd * (d - jnp.mean(d, axis=-1, keepdims=True) - xhat * jnp.mean(d * xhat, axis=-1, keepdims=True))


def gather_rows(shard):
    return lax.all_gather(shard, "fsdp", axis=0, tiled=True)


def exchange(val, bit):
    return lax.ppermute(val, "fsdp", [(i, i ^ bit) for i in range(NS)])


def pick(val, axis, index):
    return lax.dynamic_index_in_dim(val, index, axis, keepdims=False)


class Reduction:
    def __init__(self, send, keep, core, x_first, first=0):
        self.rows, self.cols = send.shape[2:]
        self.keep, self.core, self.x_first, self.first = keep, core, x_first, first
        self.near_bit, self.far_bit = (2, 4) if x_first else (4, 2)
        self.got1 = exchange(send, 1)

    def pick_yx(self, near, far):
        return (far, near) if self.x_first else (near, far)

    def term_specs(self, rows, near, far, at):
        def keep_map(s, idx):
            core = idx[2] if self.core else 0
            return (*self.pick_yx(near(s, idx), far(s, idx)), core, self.first // rows + at(s), 0)

        def got_map(s, idx):
            return (*self.pick_yx(near(s, idx), far(s, idx)), at(s), 0)

        return [(self.keep, pl.BlockSpec((None, None, None, rows, self.cols), keep_map)),
                (self.got1, pl.BlockSpec((None, None, rows, self.cols), got_map))]

    def plan(self, stage, n):
        mine = (lambda idx: idx[0], lambda idx: idx[1]) if self.x_first else (lambda idx: idx[1], lambda idx: idx[0])
        my_near, my_far = mine
        if stage == "near":
            per = n // 2
            rows = self.rows // per
            ins = self.term_specs(rows, lambda s, idx: 1 - my_near(idx), lambda s, idx: s // per, lambda s: s % per)
            return ins, (2, self.rows, self.cols), pl.BlockSpec((None, rows, self.cols), lambda s, idx: (s // per, s % per, 0))
        rows = self.rows // n
        far = (lambda s, idx: 1 - my_far(idx)) if stage == "far" else (lambda s, idx: my_far(idx))
        ins = self.term_specs(rows, lambda s, idx: my_near(idx), far, lambda s: s)
        ins.append((self.got2, pl.BlockSpec((None, rows, self.cols), lambda s, idx: (far(s, idx), s, 0))))
        flat = pl.BlockSpec((rows, self.cols), lambda s, idx: (s, 0))
        if stage == "rep":
            ins.append((self.got3, flat))
        return ins, (self.rows, self.cols), flat

    def start(self, stage, value):
        if stage == "near":
            self.got2 = exchange(value, self.near_bit)
        elif stage == "far":
            self.got3 = exchange(value, self.far_bit)
        else:
            self.part = value
            self.got4 = lax.ppermute(value, "rep", [(0, 1), (1, 0)])

    def result(self):
        return self.part + self.got4


def moves_kernel(counts, idx_ref, *refs):
    outs = refs[sum(counts):]
    at = 0
    for count, out in zip(counts, outs):
        total = refs[at][...]
        for ref in refs[at + 1:at + count]:
            total = total + ref[...]
        out[...] = total
        at += count


MOVE_STEPS = 4


def advance(anchor, *moves):
    flat = [(r, stage) for group, stage in moves for r in group]
    plans = [r.plan(stage, MOVE_STEPS) for r, stage in flat]
    me = lax.axis_index("fsdp")
    idx = jnp.stack([lax.rem(me // 2, 2), me // 4, lax.rem(me, 2)]).astype(jnp.int32)
    values = pl.pallas_call(
        functools.partial(moves_kernel, [len(ins) for ins, _, _ in plans]),
        grid_spec=pltpu.PrefetchScalarGridSpec(
            num_scalar_prefetch=1, grid=(MOVE_STEPS,),
            in_specs=[spec for ins, _, _ in plans for _, spec in ins],
            out_specs=[spec for _, _, spec in plans]),
        out_shape=[jax.ShapeDtypeStruct(shape, F32) for _, shape, _ in plans],
        compiler_params=pltpu.CompilerParams(dimension_semantics=("arbitrary",)),
        cost_estimate=pl.CostEstimate(flops=1_000_000_000, bytes_accessed=10_000_000, transcendentals=0),
        name="moves",
    )(idx, *[val for ins, _, _ in plans for val, _ in ins])
    anchor, values = lax.optimization_barrier((anchor, values))
    for (r, stage), value in zip(flat, values):
        r.start(stage, value)
    return anchor


def split_full(full, pieces):
    rows = full.shape[0] // NS
    parts = full.reshape(2, 2, 2, rows, full.shape[1])
    core = lax.rem(lax.axis_index("fsdp"), 2)
    cut = rows // pieces
    return [Reduction(pick(parts[:, :, :, i * cut:(i + 1) * cut], 2, 1 - core), parts, True, i % 2 == 0, i * cut)
            for i in range(pieces)]


def row_major(val):
    return with_layout_constraint(val, Layout(major_to_minor=tuple(range(val.ndim))))


def solution(mesh):
    batch_spec = P(("rep", "fsdp"), None, None)
    row_spec = P("fsdp", None)
    flat_spec = P("fsdp")
    col_spec = P(None, "fsdp")
    param_specs = (row_spec, flat_spec, row_spec, row_spec, flat_spec, row_spec, col_spec)

    def device_step(x_loc, dz_loc, w_qkv, b_qkv, w_out, w_up, b_up, w_down, vec_params):
        def by_half(val):
            lead = val.shape[:-1]
            return val.reshape(lead + (3, 2, HALF)).swapaxes(-3, -2).reshape(lead + (3 * D,))

        def from_half(val):
            lead = val.shape[:-1]
            return val.reshape(lead + (2, 3, HALF)).swapaxes(-3, -2).reshape(lead + (3 * D,))

        w_first = gather_rows(jnp.concatenate([by_half(w_qkv.astype(BF16)), w_out.astype(BF16)], axis=1))
        wq = w_first[:, :3 * D]
        wo = w_first[:, 3 * D:]
        up_split = w_up.reshape(D // NS, NS, CHUNKS, FC)
        down_split = w_down.reshape(CHUNKS, 2, D // NS, D)
        w_mlp = []
        for c in range(CHUNKS):
            up = up_split[:, :, c].reshape(D // NS, NS * FC).astype(BF16)
            down = jnp.concatenate([down_split[c, 0], down_split[c, 1]], axis=1).astype(BF16)
            w_mlp.append(lax.all_gather(jnp.concatenate([up, down], axis=0), "fsdp", axis=0, tiled=False))
        small = jnp.concatenate([b_qkv, b_up, vec_params.reshape(-1)]).astype(BF16)
        small = lax.all_gather(small, "fsdp", axis=0, tiled=False).astype(F32)
        nq, nu = b_qkv.shape[0], b_up.shape[0]
        bias_qkv = by_half(small[:, :nq].reshape(-1))
        bias_up = small[:, nq:nq + nu].reshape(NS, CHUNKS, FC)
        vec = small[:, nq + nu:].reshape(NS, 8, D // NS).transpose(1, 0, 2).reshape(8, D)
        ln1_gain, ln1_bias, out_bias, scale_attn, ln2_gain, ln2_bias, down_bias, scale_mlp = vec

        x_flat = row_major(x_loc.reshape(T, D))
        g_flat = row_major(dz_loc.reshape(T, D))
        x = x_flat.astype(F32)
        d_mlp_bf = row_major((g_flat.astype(F32) * scale_mlp).astype(BF16))
        d_mlp_t = d_mlp_bf.T

        xhat1, rstd1 = ln_stats(x)
        h1 = (xhat1 * ln1_gain + ln1_bias).astype(BF16)
        qkv = (dot(h1, wq) + bias_qkv).astype(BF16)
        heads = attn_forward(qkv)
        att = dot(heads, wo) + out_bias
        y = x + scale_attn * att
        xhat2, rstd2 = ln_stats(y)
        h2 = row_major((xhat2 * ln2_gain + ln2_bias).astype(BF16))
        h2_t = h2.T

        quad = lambda v: v.reshape((2, 2) + v.shape[1:])
        five = lambda v: v.reshape((2, 2, 1) + v.shape[1:])
        partial = []
        grad_bup = []
        mlp = []
        for c in range(CHUNKS):
            m_c, dh_c, up_send, up_keep, down_send, down_keep, gb = mlp_chunk(h2, d_mlp_bf, h2_t, d_mlp_t, w_mlp[c],
                                                                              bias_up[:, c].reshape(1, -1))
            mlp.append([Reduction(quad(up_send), five(up_keep), False, True),
                        Reduction(quad(down_send), five(down_keep), False, False)])
            grad_bup.append(gb.reshape(NS, FC))
            partial += [m_c, dh_c]
        partial = advance(partial, (mlp[0], "near"))
        z, g_resid, d_att_bf, vec_sums = post_mlp(partial[0], partial[2], partial[1], partial[3], x_flat, att, g_flat, vec)
        d_heads = dot_nt(d_att_bf, wo).astype(BF16)
        out_red = split_full(dot_tn(heads, d_att_bf), 2)

        d_heads = advance(d_heads, (mlp[1], "near"), (mlp[0], "far"))
        d_qkv0, gb0 = attn_backward(qkv, d_heads, 0)
        qkv0 = split_full(dot_tn(h1, d_qkv0), 2)
        d_qkv0, d_heads = advance((d_qkv0, d_heads), (out_red, "near"), (mlp[1], "far"), (mlp[0], "rep"))
        d_qkv1, gb1 = attn_backward(qkv, d_heads, 1)
        d_qkv1 = advance(d_qkv1, (qkv0, "near"), (out_red, "far"), (mlp[1], "rep"))
        qkv1 = split_full(dot_tn(h1, d_qkv1), 2)
        d_h1 = dot_nt(d_qkv0, wq[:, :3 * HALF])
        d_qkv1, d_h1 = advance((d_qkv1, d_h1), (qkv0, "far"), (out_red, "rep"))
        d_h1 = d_h1 + dot_nt(d_qkv1, wq[:, 3 * HALF:])
        d_h1 = advance(d_h1, (qkv1, "near"), (qkv0, "rep"))
        grad_ln1_gain = jnp.sum(d_h1 * xhat1, axis=0)
        grad_ln1_bias = jnp.sum(d_h1, axis=0)
        dx = (g_resid + ln_back(xhat1, rstd1, d_h1 * ln1_gain)).astype(BF16)
        grad_vec = jnp.concatenate([grad_ln1_gain[None], grad_ln1_bias[None], vec_sums[2:]], axis=0)
        grad_bqkv = from_half(jnp.sum(jnp.concatenate([gb0, gb1], axis=2), axis=(0, 1))).reshape(NS, nq)
        grad_bup = jnp.stack(grad_bup, axis=1).reshape(NS, nu)
        grad_vec = grad_vec.reshape(8, NS, D // NS).transpose(1, 0, 2).reshape(NS, D)
        small_grads = jnp.concatenate([grad_bqkv, grad_bup, grad_vec, jnp.zeros((NS, 64 * 128 - nq - nu - D), F32)], axis=1)
        small_red = split_full(small_grads.reshape(NS * 64, 128), 1)
        advance((), (qkv1, "far"), (small_red, "near"))
        advance((), (qkv1, "rep"), (small_red, "far"))
        advance((), (small_red, "rep"))
        whole = lambda group: jnp.concatenate([r.result() for r in group], axis=0)
        grad_w_out = whole(out_red)
        grad_w_qkv = from_half(jnp.concatenate([whole(qkv0), whole(qkv1)], axis=1))
        grad_up = [pair[0].result().reshape(D // NS, NS, FC) for pair in mlp]
        grad_down = [pair[1].result().T for pair in mlp]

        mine = small_red[0].result().reshape(-1)
        return (z.reshape(SEQS, SEQ, D), dx.reshape(SEQS, SEQ, D), grad_w_qkv, mine[:nq], grad_w_out,
                jnp.stack(grad_up, axis=2).reshape(D // NS, FF), mine[nq:nq + nu],
                jnp.concatenate(grad_down, axis=0), mine[nq + nu:nq + nu + D].reshape(8, D // NS))

    return jax.shard_map(device_step, mesh=mesh, in_specs=(batch_spec, batch_spec) + param_specs,
                         out_specs=(batch_spec, batch_spec) + param_specs, check_vma=False)
```

```python
import functools

import jax
import jax.numpy as jnp
from jax import lax
from jax.experimental import pallas as pl
from jax.experimental.layout import Layout, with_layout_constraint
from jax.experimental.pallas import tpu as pltpu
from jax.sharding import PartitionSpec as P


HEADS = 16
LN_EPS = 1e-5
SEQ = 50
D = 1024
FF = 4096
SEQS = 32
T = SEQS * SEQ
NS = 8
CHUNKS = 2
HALF = D // 2
FC = FF // NS // CHUNKS
GROUP = 8
ROWS = GROUP * SEQ
PAIR = 2 * SEQ
WIN = 112
SCALE = (D // HEADS) ** -0.5
NEG = -3.0e38
F32 = jnp.float32
BF16 = jnp.bfloat16

ERFC_P = 0.45
ERFC_Q = (0.25388532876968384, 0.25388315320014954, 0.22827185690402985, 0.1752501279115677, 0.11996052414178848,
          -0.0223874319344759, 0.14245237410068512, -0.30063509941101074, 0.19071702659130096, -0.041397832334041595)


def dot(a, b):
    return lax.dot_general(a, b, (((1,), (0,)), ((), ())), preferred_element_type=F32)


def dot_nt(a, b):
    return lax.dot_general(a, b, (((1,), (1,)), ((), ())), preferred_element_type=F32)


def dot_tn(a, b):
    return lax.dot_general(a, b, (((0,), (0,)), ((), ())), preferred_element_type=F32)


def gelu_and_slope(u):
    dens = jnp.exp(u * u * -0.5)
    t = 1.0 / (1.0 + (ERFC_P * 0.5 ** 0.5) * jnp.abs(u))
    q = jnp.full_like(t, ERFC_Q[-1])
    for coef in ERFC_Q[-2::-1]:
        q = q * t + coef
    half = (0.5 * dens) * (t * q)
    cdf = jnp.where(u > 0, 1.0 - half, half)
    return u * cdf, cdf + u * dens * 0.3989422804014327


def window_parts(j):
    start = 16 * ((PAIR * j) // 16)
    off = PAIR * j - start
    r = lax.broadcasted_iota(jnp.int32, (WIN, WIN), 0)
    c = lax.broadcasted_iota(jnp.int32, (WIN, WIN), 1)

    def seq_of(v):
        one = jnp.int32(1)
        zero = jnp.int32(0)
        return (jnp.where(v >= off, one, zero) + jnp.where(v >= off + SEQ, one, zero)
                + jnp.where(v >= off + PAIR, one, zero))

    bias = jnp.where(seq_of(r) == seq_of(c), 0.0, NEG)
    row = lax.broadcasted_iota(jnp.int32, (WIN, 128), 0)
    lane = lax.broadcasted_iota(jnp.int32, (WIN, 128), 1)
    inside = (row >= off) & (row < off + PAIR)
    return start, bias, inside, lane < 64


def softmax_rows(s, bias2):
    s = jnp.where(bias2 == 0.0, s, NEG)
    m = jnp.max(s, axis=1, keepdims=True)
    p = jnp.exp((s - m) * SCALE)
    return p * (1.0 / jnp.sum(p, axis=1, keepdims=True))


def attn_fwd_kernel(q_ref, k_ref, v_ref, o_ref):
    for j in range(ROWS // PAIR):
        start, bias, inside, even = window_parts(j)
        bias2 = jnp.concatenate([bias, bias], axis=0)
        m_even = jnp.where(even, 1.0, 0.0).astype(BF16)
        m_odd = jnp.where(even, 0.0, 1.0).astype(BF16)
        for hp in range(q_ref.shape[1] // 128):
            cols = slice(hp * 128, hp * 128 + 128)
            q = q_ref[start:start + WIN, cols]
            k = k_ref[start:start + WIN, cols]
            v = v_ref[start:start + WIN, cols]
            q2 = jnp.concatenate([q * m_even, q * m_odd], axis=0)
            p = softmax_rows(dot_nt(q2, k), bias2)
            o2 = dot(p.astype(BF16), v)
            o = jnp.where(inside, jnp.where(even, o2[:WIN], o2[WIN:]), 0.0).astype(BF16)
            if j:
                o_ref[start:start + 16, cols] += o[:16]
                o_ref[start + 16:start + WIN, cols] = o[16:]
            else:
                o_ref[start:start + WIN, cols] = o


def attn_bwd_kernel(q_ref, k_ref, v_ref, g_ref, d_ref, b_ref):
    parts = []
    for j in range(ROWS // PAIR):
        start, bias, inside, even = window_parts(j)
        one_even = jnp.where(even, 1.0, 0.0)
        parts.append((start, jnp.concatenate([bias, bias], axis=0), one_even.astype(BF16), (1.0 - one_even).astype(BF16),
                      jnp.where(inside, one_even, 0.0).astype(BF16), jnp.where(inside, 1.0 - one_even, 0.0).astype(BF16)))

    def head_pair(hp, carry):
        cols = pl.ds(pl.multiple_of(hp * 128, 128), 128)
        sums = [jnp.zeros((1, 128), F32) for _ in range(3)]
        for j, (start, bias2, m_even, m_odd, g_even, g_odd) in enumerate(parts):
            q = q_ref[start:start + WIN, cols]
            k = k_ref[start:start + WIN, cols]
            v = v_ref[start:start + WIN, cols]
            g = g_ref[start:start + WIN, cols]
            q2 = jnp.concatenate([q * m_even, q * m_odd], axis=0)
            g2 = jnp.concatenate([g * g_even, g * g_odd], axis=0)
            p = softmax_rows(dot_nt(q2, k), bias2)
            dp = dot_nt(g2, v)
            ds = (p * (dp - jnp.sum(dp * p, axis=1, keepdims=True)) * SCALE).astype(BF16)
            dq2 = dot(ds, k)
            even = lax.broadcasted_iota(jnp.int32, (WIN, 128), 1) < 64
            dq = jnp.where(even, dq2[:WIN], dq2[WIN:])
            dk = dot_tn(ds, q2)
            dv = dot_tn(p.astype(BF16), g2)
            for i, val in enumerate((dq, dk, dv)):
                out = pl.ds(pl.multiple_of(hp * 128 + i * HALF, 128), 128)
                sums[i] = sums[i] + jnp.sum(val, axis=0, keepdims=True)
                val = val.astype(BF16)
                if j:
                    d_ref[start:start + 16, out] += val[:16]
                    d_ref[start + 16:start + WIN, out] = val[16:]
                else:
                    d_ref[start:start + WIN, out] = val
        for i in range(3):
            b_ref[0, :, pl.ds(pl.multiple_of(hp * 128 + i * HALF, 128), 128)] = sums[i]
        return carry

    lax.fori_loop(0, HALF // 128, head_pair, 0)


ATT_COLS = 256


def attn_forward(qkv):
    per = HALF // ATT_COLS
    spec = lambda part: pl.BlockSpec((ROWS, ATT_COLS), lambda g, c: (g, (c // per * 3 + part) * per + c % per))
    return pl.pallas_call(
        attn_fwd_kernel,
        grid=(T // ROWS, D // ATT_COLS),
        in_specs=[spec(0), spec(1), spec(2)],
        out_specs=pl.BlockSpec((ROWS, ATT_COLS), lambda g, c: (g, c)),
        out_shape=jax.ShapeDtypeStruct((T, D), BF16),
        compiler_params=pltpu.CompilerParams(dimension_semantics=("arbitrary", "arbitrary")),
        cost_estimate=pl.CostEstimate(flops=8_000_000_000, bytes_accessed=13_000_000, transcendentals=3_000_000),
        name="attn_fwd",
    )(qkv, qkv, qkv)


def attn_backward(qkv, d_heads, half):
    spec = lambda at: pl.BlockSpec((ROWS, HALF), lambda g: (g, at))
    return pl.pallas_call(
        attn_bwd_kernel,
        grid=(T // ROWS,),
        in_specs=[spec(3 * half), spec(3 * half + 1), spec(3 * half + 2), spec(half)],
        out_specs=[pl.BlockSpec((ROWS, 3 * HALF), lambda g: (g, 0)), pl.BlockSpec((1, 1, 3 * HALF), lambda g: (g, 0, 0))],
        out_shape=[jax.ShapeDtypeStruct((T, 3 * HALF), BF16), jax.ShapeDtypeStruct((T // ROWS, 1, 3 * HALF), F32)],
        compiler_params=pltpu.CompilerParams(dimension_semantics=("arbitrary",)),
        cost_estimate=pl.CostEstimate(flops=16_000_000_000, bytes_accessed=12_000_000, transcendentals=1_500_000),
        name="attn_bwd",
    )(qkv, qkv, qkv, d_heads)


MLP_ROWS = 400
BLK = 2 * FC


def mlp_kernel(h_ref, g_ref, ht_send, ht_keep, gt_ref, w1_ref, wd_ref, b1_ref, m_ref, dh_ref,
               gw1_send, gw1_keep, gw2_send, gw2_keep, gb_ref, act_s, dpre_s, w2_ref):
    step = pl.program_id(0)
    core = lax.rem(lax.axis_index("fsdp"), 2)
    for n in range(4):
        w2_ref[n * 128:(n + 1) * 128, :] = wd_ref[n // 2, :, n % 2 * D:(n % 2 + 1) * D]

    @pl.when(step == 0)
    def _():
        m_ref[...] = jnp.zeros_like(m_ref)
        dh_ref[...] = jnp.zeros_like(dh_ref)

    tiles = [(i, n) for i in range(T // MLP_ROWS) for n in range(2)]
    sums = [jnp.zeros((1, FC), F32) for _ in range(2)]

    def products(i, n):
        rows = slice(i * MLP_ROWS, (i + 1) * MLP_ROWS)
        cols = slice(n * FC, (n + 1) * FC)
        u = dot(h_ref[rows, :], w1_ref[:, :, cols].reshape(D, FC))
        return u, dot_nt(g_ref[rows, :], w2_ref[cols, :])

    def activation(i, n, u, d_act):
        rows = slice(i * MLP_ROWS, (i + 1) * MLP_ROWS)
        cols = slice(n * FC, (n + 1) * FC)
        act, slope = gelu_and_slope(u + b1_ref[:, cols])
        d_pre = d_act * slope
        sums[n] = sums[n] + jnp.sum(d_pre, axis=0, keepdims=True)
        act_s[n, rows, :] = act.astype(BF16)
        dpre_s[rows, cols] = d_pre.astype(BF16)

    def outputs(i):
        rows = slice(i * MLP_ROWS, (i + 1) * MLP_ROWS)
        m_ref[rows, :] += dot(act_s[0, rows, :], w2_ref[:FC, :]) + dot(act_s[1, rows, :], w2_ref[FC:, :])
        dh_ref[rows, :] += dot_nt(dpre_s[rows, :], w1_ref[...].reshape(D, BLK))

    held = None
    for at, (i, n) in enumerate(tiles):
        fresh = products(i, n)
        if held is not None:
            activation(*tiles[at - 1], *held)
        if n == 1 and i > 0:
            outputs(i - 1)
        held = fresh
    activation(*tiles[-1], *held)
    outputs(T // MLP_ROWS - 1)
    gb_ref[:, :FC] = sums[0]
    gb_ref[:, FC:] = sums[1]

    for src, out in ((ht_send, gw1_send), (ht_keep, gw1_keep)):
        out[...] = dot(src[...].reshape(D // 2, T), dpre_s[...]).reshape(4, D // NS, BLK)
    gw2_send[0] = dot(gt_ref[...], act_s[1 - core])
    gw2_keep[0] = dot(gt_ref[...], act_s[core])


def mlp_chunk(h, g, ht, gt, weights, b1):
    cols = NS * FC
    once = pl.Buffered(1)
    whole = lambda shape: pl.BlockSpec(shape, lambda s: (0, 0), pipeline_mode=once)
    core = lambda: lax.rem(lax.axis_index("fsdp"), 2)
    half = lambda side: pl.BlockSpec((4, None, D // NS, T), lambda s: (0, side(), 0, 0), pipeline_mode=once)
    ht = ht.reshape(4, 2, D // NS, T)
    return pl.pallas_call(
        mlp_kernel,
        grid=(cols // BLK,),
        in_specs=[whole((T, D)), whole((T, D)), half(lambda: 1 - core()), half(core), whole((D, T)),
                  pl.BlockSpec((NS, D // NS, BLK), lambda s: (0, 0, s)),
                  pl.BlockSpec((2, D // NS, cols), lambda s: (s, 1, 0)),
                  pl.BlockSpec((1, BLK), lambda s: (0, s))],
        out_specs=[whole((T, D)), whole((T, D)),
                   *[pl.BlockSpec((4, D // NS, BLK), lambda s: (0, 0, s))] * 2,
                   *[pl.BlockSpec((1, D, FC), lambda s: (s, 0, 0))] * 2,
                   pl.BlockSpec((1, BLK), lambda s: (0, s))],
        out_shape=[jax.ShapeDtypeStruct((T, D), F32), jax.ShapeDtypeStruct((T, D), F32),
                   *[jax.ShapeDtypeStruct((4, D // NS, cols), F32)] * 2, *[jax.ShapeDtypeStruct((4, D, FC), F32)] * 2,
                   jax.ShapeDtypeStruct((1, cols), F32)],
        scratch_shapes=[pltpu.VMEM((2, T, FC), BF16), pltpu.VMEM((T, BLK), BF16), pltpu.VMEM((BLK, D), BF16)],
        compiler_params=pltpu.CompilerParams(dimension_semantics=("arbitrary",), vmem_limit_bytes=62 * 1024 * 1024),
        cost_estimate=pl.CostEstimate(flops=12 * T * D * cols, bytes_accessed=60_000_000, transcendentals=T * cols),
        name="mlp_fwd_bwd",
    )(h, g, ht, ht, gt, weights, weights, b1)


POST_ROWS = 200


def post_kernel(m0_ref, m1_ref, d0_ref, d1_ref, x_ref, att_ref, g_ref, vec_ref, z_ref, res_ref, da_ref, sum_ref):
    row = lambda i: vec_ref[i:i + 1, :]
    att = att_ref[...]
    y = x_ref[...].astype(F32) + row(3) * att
    m = m0_ref[...] + m1_ref[...] + row(6)
    g = g_ref[...].astype(F32)
    z_ref[...] = (y + row(7) * m).astype(BF16)
    xhat, rstd = ln_stats(y)
    dh = d0_ref[...] + d1_ref[...]
    res = g + ln_back(xhat, rstd, dh * row(4))
    res_ref[...] = res
    da = res * row(3)
    da_ref[...] = da.astype(BF16)

    @pl.when(pl.program_id(0) == 0)
    def _():
        sum_ref[...] = jnp.zeros_like(sum_ref)

    for i, val in ((2, da), (3, res * att), (4, dh * xhat), (5, dh), (6, g * row(7)), (7, g * m)):
        sum_ref[i:i + 1, :] += jnp.sum(val, axis=0, keepdims=True)


def post_mlp(m0, m1, d0, d1, x, att, g, vec):
    rows = pl.BlockSpec((POST_ROWS, D), lambda i: (i, 0))
    fixed = pl.BlockSpec((8, D), lambda i: (0, 0))
    return pl.pallas_call(
        post_kernel,
        grid=(T // POST_ROWS,),
        in_specs=[rows] * 7 + [fixed],
        out_specs=[rows, rows, rows, fixed],
        out_shape=[jax.ShapeDtypeStruct((T, D), BF16), jax.ShapeDtypeStruct((T, D), F32), jax.ShapeDtypeStruct((T, D), BF16),
                   jax.ShapeDtypeStruct((8, D), F32)],
        compiler_params=pltpu.CompilerParams(dimension_semantics=("arbitrary",)),
        cost_estimate=pl.CostEstimate(flops=5_000_000_000, bytes_accessed=56_000_000, transcendentals=T),
        name="post_mlp",
    )(m0, m1, d0, d1, x, att, g, vec)


def ln_stats(t):
    mean = jnp.mean(t, axis=-1, keepdims=True)
    centered = t - mean
    variance = jnp.mean(centered * centered, axis=-1, keepdims=True)
    rstd = lax.rsqrt(variance + LN_EPS)
    return centered * rstd, rstd


def ln_back(xhat, rstd, d):
    return rstd * (d - jnp.mean(d, axis=-1, keepdims=True) - xhat * jnp.mean(d * xhat, axis=-1, keepdims=True))


LN1_ROWS = 400


def ln1_kernel(d0_ref, d1_ref, w_ref, x_ref, res_ref, vec_ref, dx_ref, sum_ref):
    dh = dot_nt(d0_ref[...], w_ref[:, :3 * HALF]) + dot_nt(d1_ref[...], w_ref[:, 3 * HALF:])
    xhat, rstd = ln_stats(x_ref[...].astype(F32))
    dx_ref[...] = (res_ref[...] + ln_back(xhat, rstd, dh * vec_ref[0:1, :])).astype(BF16)

    @pl.when(pl.program_id(0) == 0)
    def _():
        sum_ref[...] = jnp.zeros_like(sum_ref)

    sum_ref[0:1, :] += jnp.sum(dh * xhat, axis=0, keepdims=True)
    sum_ref[1:2, :] += jnp.sum(dh, axis=0, keepdims=True)


def ln1_backward(d0, d1, w_first, x, res, vec):
    rows = pl.BlockSpec((LN1_ROWS, D), lambda i: (i, 0))
    fixed = pl.BlockSpec((8, D), lambda i: (0, 0))
    return pl.pallas_call(
        ln1_kernel,
        grid=(T // LN1_ROWS,),
        in_specs=[pl.BlockSpec((LN1_ROWS, 3 * HALF), lambda i: (i, 0))] * 2
        + [pl.BlockSpec((D, 3 * D), lambda i: (0, 0), pipeline_mode=pl.Buffered(1)), rows, rows, fixed],
        out_specs=[rows, fixed],
        out_shape=[jax.ShapeDtypeStruct((T, D), BF16), jax.ShapeDtypeStruct((8, D), F32)],
        compiler_params=pltpu.CompilerParams(dimension_semantics=("arbitrary",)),
        cost_estimate=pl.CostEstimate(flops=6 * T * D * D, bytes_accessed=30_000_000, transcendentals=T),
        name="ln1_back",
    )(d0, d1, w_first, x, res, vec)


def gather_rows(shard):
    return lax.all_gather(shard, "fsdp", axis=0, tiled=True)


def exchange(val, bit):
    return lax.ppermute(val, "fsdp", [(i, i ^ bit) for i in range(NS)])


def pick(val, axis, index):
    return lax.dynamic_index_in_dim(val, index, axis, keepdims=False)


class Reduction:
    def __init__(self, send, keep, core, x_first, first=0):
        self.rows, self.cols = send.shape[2:]
        self.keep, self.core, self.x_first, self.first = keep, core, x_first, first
        self.near_bit, self.far_bit = (2, 4) if x_first else (4, 2)
        self.got1 = exchange(send, 1)

    def pick_yx(self, near, far):
        return (far, near) if self.x_first else (near, far)

    def term_specs(self, rows, near, far, at):
        def keep_map(s, idx):
            core = idx[2] if self.core else 0
            return (*self.pick_yx(near(s, idx), far(s, idx)), core, self.first // rows + at(s), 0)

        def got_map(s, idx):
            return (*self.pick_yx(near(s, idx), far(s, idx)), at(s), 0)

        return [(self.keep, pl.BlockSpec((None, None, None, rows, self.cols), keep_map)),
                (self.got1, pl.BlockSpec((None, None, rows, self.cols), got_map))]

    def plan(self, stage, n):
        mine = (lambda idx: idx[0], lambda idx: idx[1]) if self.x_first else (lambda idx: idx[1], lambda idx: idx[0])
        my_near, my_far = mine
        if stage == "near":
            per = n // 2
            rows = self.rows // per
            ins = self.term_specs(rows, lambda s, idx: 1 - my_near(idx), lambda s, idx: s // per, lambda s: s % per)
            return ins, (2, self.rows, self.cols), pl.BlockSpec((None, rows, self.cols), lambda s, idx: (s // per, s % per, 0))
        rows = self.rows // n
        far = (lambda s, idx: 1 - my_far(idx)) if stage == "far" else (lambda s, idx: my_far(idx))
        ins = self.term_specs(rows, lambda s, idx: my_near(idx), far, lambda s: s)
        ins.append((self.got2, pl.BlockSpec((None, rows, self.cols), lambda s, idx: (far(s, idx), s, 0))))
        flat = pl.BlockSpec((rows, self.cols), lambda s, idx: (s, 0))
        if stage == "rep":
            ins.append((self.got3, flat))
        return ins, (self.rows, self.cols), flat

    def start(self, stage, value):
        if stage == "near":
            self.got2 = exchange(value, self.near_bit)
        elif stage == "far":
            self.got3 = exchange(value, self.far_bit)
        else:
            self.part = value
            self.got4 = lax.ppermute(value, "rep", [(0, 1), (1, 0)])

    def result(self):
        return self.part + self.got4


def moves_kernel(counts, idx_ref, *refs):
    outs = refs[sum(counts):]
    at = 0
    for count, out in zip(counts, outs):
        total = refs[at][...]
        for ref in refs[at + 1:at + count]:
            total = total + ref[...]
        out[...] = total
        at += count


MOVE_STEPS = 4


def advance(anchor, *moves):
    flat = [(r, stage) for group, stage in moves for r in group]
    plans = [r.plan(stage, MOVE_STEPS) for r, stage in flat]
    me = lax.axis_index("fsdp")
    idx = jnp.stack([lax.rem(me // 2, 2), me // 4, lax.rem(me, 2)]).astype(jnp.int32)
    values = pl.pallas_call(
        functools.partial(moves_kernel, [len(ins) for ins, _, _ in plans]),
        grid_spec=pltpu.PrefetchScalarGridSpec(
            num_scalar_prefetch=1, grid=(MOVE_STEPS,),
            in_specs=[spec for ins, _, _ in plans for _, spec in ins],
            out_specs=[spec for _, _, spec in plans]),
        out_shape=[jax.ShapeDtypeStruct(shape, F32) for _, shape, _ in plans],
        compiler_params=pltpu.CompilerParams(dimension_semantics=("arbitrary",)),
        cost_estimate=pl.CostEstimate(flops=1_000_000_000, bytes_accessed=10_000_000, transcendentals=0),
        name="moves",
    )(idx, *[val for ins, _, _ in plans for val, _ in ins])
    anchor, values = lax.optimization_barrier((anchor, values))
    for (r, stage), value in zip(flat, values):
        r.start(stage, value)
    return anchor


def split_full(full, pieces):
    rows = full.shape[0] // NS
    parts = full.reshape(2, 2, 2, rows, full.shape[1])
    core = lax.rem(lax.axis_index("fsdp"), 2)
    cut = rows // pieces
    return [Reduction(pick(parts[:, :, :, i * cut:(i + 1) * cut], 2, 1 - core), parts, True, i % 2 == 0, i * cut)
            for i in range(pieces)]


def row_major(val):
    return with_layout_constraint(val, Layout(major_to_minor=tuple(range(val.ndim))))


def solution(mesh):
    batch_spec = P(("rep", "fsdp"), None, None)
    row_spec = P("fsdp", None)
    flat_spec = P("fsdp")
    col_spec = P(None, "fsdp")
    param_specs = (row_spec, flat_spec, row_spec, row_spec, flat_spec, row_spec, col_spec)

    def layer_step(x_loc, dz_loc, w_qkv, b_qkv, w_out, w_up, b_up, w_down, vec_params):
        def by_half(val):
            lead = val.shape[:-1]
            return val.reshape(lead + (3, 2, HALF)).swapaxes(-3, -2).reshape(lead + (3 * D,))

        def from_half(val):
            lead = val.shape[:-1]
            return val.reshape(lead + (2, 3, HALF)).swapaxes(-3, -2).reshape(lead + (3 * D,))

        w_first = row_major(jnp.concatenate([by_half(w_qkv.astype(BF16)), w_out.astype(BF16)], axis=1))
        w_first = row_major(gather_rows(w_first))
        wq = w_first[:, :3 * D]
        wo = w_first[:, 3 * D:]
        up_split = w_up.reshape(D // NS, NS, CHUNKS, FC)
        down_split = w_down.reshape(CHUNKS, 2, D // NS, D)
        w_mlp = []
        for c in range(CHUNKS):
            up = up_split[:, :, c].reshape(D // NS, NS * FC).astype(BF16)
            down = jnp.concatenate([down_split[c, 0], down_split[c, 1]], axis=1).astype(BF16)
            shard = row_major(jnp.concatenate([up, down], axis=0))
            w_mlp.append(row_major(lax.all_gather(shard, "fsdp", axis=0, tiled=False)))
        small = jnp.concatenate([b_qkv, b_up, vec_params.reshape(-1)]).astype(BF16)
        small = lax.all_gather(small, "fsdp", axis=0, tiled=False).astype(F32)
        nq, nu = b_qkv.shape[0], b_up.shape[0]
        bias_qkv = by_half(small[:, :nq].reshape(-1))
        bias_up = small[:, nq:nq + nu].reshape(NS, CHUNKS, FC)
        vec = small[:, nq + nu:].reshape(NS, 8, D // NS).transpose(1, 0, 2).reshape(8, D)
        ln1_gain, ln1_bias, out_bias, scale_attn, ln2_gain, ln2_bias, _, scale_mlp = vec

        x_flat = row_major(x_loc.reshape(T, D))
        g_flat = row_major(dz_loc.reshape(T, D))
        x = x_flat.astype(F32)
        d_mlp_bf = row_major((g_flat.astype(F32) * scale_mlp).astype(BF16))
        d_mlp_t = d_mlp_bf.T

        xhat1, _ = ln_stats(x)
        h1 = (xhat1 * ln1_gain + ln1_bias).astype(BF16)
        qkv = (dot(h1, wq) + bias_qkv).astype(BF16)
        heads = attn_forward(qkv)
        att = dot(heads, wo) + out_bias
        y = x + scale_attn * att
        xhat2, _ = ln_stats(y)
        h2 = row_major((xhat2 * ln2_gain + ln2_bias).astype(BF16))
        h2_t = h2.T

        quad = lambda v: v.reshape((2, 2) + v.shape[1:])
        five = lambda v: v.reshape((2, 2, 1) + v.shape[1:])
        partial = []
        grad_bup = []
        mlp = []
        for c in range(CHUNKS):
            m_c, dh_c, up_send, up_keep, down_send, down_keep, gb = mlp_chunk(
                h2, d_mlp_bf, h2_t, d_mlp_t, w_mlp[c], bias_up[:, c].reshape(1, -1))
            mlp.append([Reduction(quad(up_send), five(up_keep), False, True),
                        Reduction(quad(down_send), five(down_keep), False, False)])
            grad_bup.append(gb.reshape(NS, FC))
            partial += [m_c, dh_c]
        partial = advance(partial, (mlp[0], "near"))
        z, g_resid, d_att_bf, vec_sums = post_mlp(partial[0], partial[2], partial[1], partial[3], x_flat, att, g_flat, vec)
        d_heads = dot_nt(d_att_bf, wo).astype(BF16)
        out_red = split_full(dot_tn(heads, d_att_bf), 2)

        d_heads = advance(d_heads, (mlp[1], "near"), (mlp[0], "far"))
        d_qkv0, gb0 = attn_backward(qkv, d_heads, 0)
        qkv0 = split_full(dot_tn(h1, d_qkv0), 2)
        d_heads = advance(d_heads, (out_red, "near"), (mlp[1], "far"), (mlp[0], "rep"))
        d_qkv1, gb1 = attn_backward(qkv, d_heads, 1)
        gw1 = dot_tn(h1, d_qkv1)
        qkv1 = split_full(gw1, 2)
        d_qkv1, z = advance((d_qkv1, z), (qkv0, "near"), (out_red, "far"), (mlp[1], "rep"))
        dx, ln1_sums = ln1_backward(d_qkv0, d_qkv1, w_first, x_flat, g_resid, vec)
        grad_vec = jnp.concatenate([ln1_sums[:2], vec_sums[2:]], axis=0)
        grad_bqkv = from_half(jnp.sum(jnp.concatenate([gb0, gb1], axis=2), axis=(0, 1))).reshape(NS, nq)
        grad_bup = jnp.stack(grad_bup, axis=1).reshape(NS, nu)
        grad_vec = grad_vec.reshape(8, NS, D // NS).transpose(1, 0, 2).reshape(NS, D)
        small_grads = jnp.concatenate([grad_bqkv, grad_bup, grad_vec, jnp.zeros((NS, 64 * 128 - nq - nu - D), F32)], axis=1)
        small_red = split_full(small_grads.reshape(NS * 64, 128), 1)
        z, dx = advance((z, dx), (qkv1, "near"), (qkv0, "far"), (out_red, "rep"))
        z = row_major(z.reshape(SEQS, SEQ, D))
        dx = advance(dx, (qkv1, "far"), (qkv0, "rep"), (small_red, "near"))
        dx = row_major(dx.reshape(SEQS, SEQ, D))
        advance((), (qkv1, "rep"), (small_red, "far"))
        advance((), (small_red, "rep"))
        whole = lambda group: jnp.concatenate([r.result() for r in group], axis=0)
        grad_w_out = whole(out_red)
        grad_w_qkv = from_half(jnp.concatenate([whole(qkv0), whole(qkv1)], axis=1))
        grad_up = [pair[0].result().reshape(D // NS, NS, FC) for pair in mlp]
        grad_down = [pair[1].result().T for pair in mlp]

        mine = small_red[0].result().reshape(-1)
        return (z, dx, grad_w_qkv, mine[:nq], grad_w_out,
                jnp.stack(grad_up, axis=2).reshape(D // NS, FF), mine[nq:nq + nu],
                jnp.concatenate(grad_down, axis=0), mine[nq + nu:nq + nu + D].reshape(8, D // NS))

    return jax.shard_map(layer_step, mesh=mesh, in_specs=(batch_spec, batch_spec) + param_specs,
                         out_specs=(batch_spec, batch_spec) + param_specs, check_vma=False)
```

```python
import functools

import jax
import jax.numpy as jnp
from jax import lax
from jax.experimental import pallas as pl
from jax.experimental.layout import Layout, with_layout_constraint
from jax.experimental.pallas import tpu as pltpu
from jax.sharding import PartitionSpec as P


HEADS = 16
LN_EPS = 1e-5
SEQ = 50
D = 1024
FF = 4096
SEQS = 32
T = SEQS * SEQ
NS = 8
CHUNKS = 2
HALF = D // 2
FC = FF // NS // CHUNKS
GROUP = 8
ROWS = GROUP * SEQ
PAIR = 2 * SEQ
WIN = 112
SCALE = (D // HEADS) ** -0.5
NEG = -3.0e38
F32 = jnp.float32
BF16 = jnp.bfloat16

ERFC_P = 0.45
ERFC_Q = (0.25388532876968384, 0.25388315320014954, 0.22827185690402985, 0.1752501279115677, 0.11996052414178848,
          -0.0223874319344759, 0.14245237410068512, -0.30063509941101074, 0.19071702659130096, -0.041397832334041595)


def dot(a, b):
    return lax.dot_general(a, b, (((1,), (0,)), ((), ())), preferred_element_type=F32)


def dot_nt(a, b):
    return lax.dot_general(a, b, (((1,), (1,)), ((), ())), preferred_element_type=F32)


def dot_tn(a, b):
    return lax.dot_general(a, b, (((0,), (0,)), ((), ())), preferred_element_type=F32)


def gelu_and_slope(u):
    dens = jnp.exp(u * u * -0.5)
    t = 1.0 / (1.0 + (ERFC_P * 0.5 ** 0.5) * jnp.abs(u))
    q = jnp.full_like(t, ERFC_Q[-1])
    for coef in ERFC_Q[-2::-1]:
        q = q * t + coef
    half = (0.5 * dens) * (t * q)
    cdf = jnp.where(u > 0, 1.0 - half, half)
    return u * cdf, cdf + u * dens * 0.3989422804014327


def window_parts(j):
    start = 16 * ((PAIR * j) // 16)
    off = PAIR * j - start
    r = lax.broadcasted_iota(jnp.int32, (WIN, WIN), 0)
    c = lax.broadcasted_iota(jnp.int32, (WIN, WIN), 1)

    def seq_of(v):
        one = jnp.int32(1)
        zero = jnp.int32(0)
        return (jnp.where(v >= off, one, zero) + jnp.where(v >= off + SEQ, one, zero)
                + jnp.where(v >= off + PAIR, one, zero))

    bias = jnp.where(seq_of(r) == seq_of(c), 0.0, NEG)
    row = lax.broadcasted_iota(jnp.int32, (WIN, 128), 0)
    lane = lax.broadcasted_iota(jnp.int32, (WIN, 128), 1)
    inside = (row >= off) & (row < off + PAIR)
    return start, bias, inside, lane < 64


def softmax_rows(s, bias2):
    s = jnp.where(bias2 == 0.0, s, NEG)
    m = jnp.max(s, axis=1, keepdims=True)
    p = jnp.exp2((s - m) * (SCALE * 1.4426950408889634))
    return p * (1.0 / jnp.sum(p, axis=1, keepdims=True))


def attn_fwd_kernel(q_ref, k_ref, v_ref, o_ref):
    for j in range(ROWS // PAIR):
        start, bias, inside, even = window_parts(j)
        bias2 = jnp.concatenate([bias, bias], axis=0)
        m_even = jnp.where(even, 1.0, 0.0).astype(BF16)
        m_odd = jnp.where(even, 0.0, 1.0).astype(BF16)
        for hp in range(q_ref.shape[1] // 128):
            cols = slice(hp * 128, hp * 128 + 128)
            q = q_ref[start:start + WIN, cols]
            k = k_ref[start:start + WIN, cols]
            v = v_ref[start:start + WIN, cols]
            q2 = jnp.concatenate([q * m_even, q * m_odd], axis=0)
            p = softmax_rows(dot_nt(q2, k), bias2)
            o2 = dot(p.astype(BF16), v)
            o = jnp.where(inside, jnp.where(even, o2[:WIN], o2[WIN:]), 0.0).astype(BF16)
            if j:
                o_ref[start:start + 16, cols] += o[:16]
                o_ref[start + 16:start + WIN, cols] = o[16:]
            else:
                o_ref[start:start + WIN, cols] = o


def attn_bwd_kernel(q_ref, k_ref, v_ref, g_ref, d_ref, b_ref):
    parts = []
    for j in range(ROWS // PAIR):
        start, bias, inside, even = window_parts(j)
        one_even = jnp.where(even, 1.0, 0.0)
        parts.append((start, jnp.concatenate([bias, bias], axis=0), one_even.astype(BF16), (1.0 - one_even).astype(BF16),
                      jnp.where(inside, one_even, 0.0).astype(BF16), jnp.where(inside, 1.0 - one_even, 0.0).astype(BF16)))

    def head_pair(hp):
        cols = slice(hp * 128, hp * 128 + 128)
        sums = [jnp.zeros((1, 128), F32) for _ in range(3)]
        for j, (start, bias2, m_even, m_odd, g_even, g_odd) in enumerate(parts):
            q = q_ref[start:start + WIN, cols]
            k = k_ref[start:start + WIN, cols]
            v = v_ref[start:start + WIN, cols]
            g = g_ref[start:start + WIN, cols]
            q2 = jnp.concatenate([q * m_even, q * m_odd], axis=0)
            g2 = jnp.concatenate([g * g_even, g * g_odd], axis=0)
            p = softmax_rows(dot_nt(q2, k), bias2)
            dp = dot_nt(g2, v)
            ds = (p * (dp - jnp.sum(dp * p, axis=1, keepdims=True)) * SCALE).astype(BF16)
            dq2 = dot(ds, k)
            even = lax.broadcasted_iota(jnp.int32, (WIN, 128), 1) < 64
            dq = jnp.where(even, dq2[:WIN], dq2[WIN:])
            dk = dot_tn(ds, q2)
            dv = dot_tn(p.astype(BF16), g2)
            for i, val in enumerate((dq, dk, dv)):
                out = slice(hp * 128 + i * HALF, hp * 128 + i * HALF + 128)
                sums[i] = sums[i] + jnp.sum(val, axis=0, keepdims=True)
                val = val.astype(BF16)
                if j:
                    d_ref[start:start + 16, out] += val[:16]
                    d_ref[start + 16:start + WIN, out] = val[16:]
                else:
                    d_ref[start:start + WIN, out] = val
        for i in range(3):
            b_ref[0, :, hp * 128 + i * HALF:hp * 128 + i * HALF + 128] = sums[i]

    for hp in range(HALF // 128):
        head_pair(hp)


ATT_COLS = 256


def attn_forward(qkv):
    per = HALF // ATT_COLS
    spec = lambda part: pl.BlockSpec((ROWS, ATT_COLS), lambda g, c: (g, (c // per * 3 + part) * per + c % per))
    return pl.pallas_call(
        attn_fwd_kernel,
        grid=(T // ROWS, D // ATT_COLS),
        in_specs=[spec(0), spec(1), spec(2)],
        out_specs=pl.BlockSpec((ROWS, ATT_COLS), lambda g, c: (g, c)),
        out_shape=jax.ShapeDtypeStruct((T, D), BF16),
        compiler_params=pltpu.CompilerParams(dimension_semantics=("arbitrary", "arbitrary")),
        cost_estimate=pl.CostEstimate(flops=8_000_000_000, bytes_accessed=13_000_000, transcendentals=3_000_000),
        name="attn_fwd",
    )(qkv, qkv, qkv)


def attn_backward(qkv, d_heads, half):
    spec = lambda at: pl.BlockSpec((ROWS, HALF), lambda g: (g, at))
    return pl.pallas_call(
        attn_bwd_kernel,
        grid=(T // ROWS,),
        in_specs=[spec(3 * half), spec(3 * half + 1), spec(3 * half + 2), spec(half)],
        out_specs=[pl.BlockSpec((ROWS, 3 * HALF), lambda g: (g, 0)), pl.BlockSpec((1, 1, 3 * HALF), lambda g: (g, 0, 0))],
        out_shape=[jax.ShapeDtypeStruct((T, 3 * HALF), BF16), jax.ShapeDtypeStruct((T // ROWS, 1, 3 * HALF), F32)],
        compiler_params=pltpu.CompilerParams(dimension_semantics=("arbitrary",)),
        cost_estimate=pl.CostEstimate(flops=16_000_000_000, bytes_accessed=12_000_000, transcendentals=1_500_000),
        name="attn_bwd",
    )(qkv, qkv, qkv, d_heads)


MLP_ROWS = 400
BLK = 2 * FC


def mlp_kernel(h_ref, g_ref, ht_ref, gt_ref, w1_ref, wd_ref, b1_ref, m_ref, dh_ref,
               gw1_send, gw1_keep, gw2_send, gw2_keep, gb_ref, act_s, dpre_s, w2_ref):
    step = pl.program_id(0)
    core = lax.rem(lax.axis_index("fsdp"), 2)
    gb_ref[...] = jnp.zeros_like(gb_ref)
    for n in range(4):
        w2_ref[n * 128:(n + 1) * 128, :] = wd_ref[n // 2, :, n % 2 * D:(n % 2 + 1) * D]

    @pl.when(step == 0)
    def _():
        m_ref[...] = jnp.zeros_like(m_ref)
        dh_ref[...] = jnp.zeros_like(dh_ref)

    def rows_step(i, carry):
        rows = pl.ds(pl.multiple_of(i * MLP_ROWS, 16), MLP_ROWS)
        w1 = w1_ref[...].reshape(D, BLK)
        u = dot(h_ref[rows, :], w1) + b1_ref[...]
        d_act = dot_nt(g_ref[rows, :], w2_ref[...])
        act, slope = gelu_and_slope(u)
        act = act.astype(BF16)
        d_pre = d_act * slope
        gb_ref[...] += jnp.sum(d_pre, axis=0, keepdims=True)
        d_pre = d_pre.astype(BF16)
        act_s[rows, :] = act
        dpre_s[rows, :] = d_pre
        m_ref[rows, :] += dot(act, w2_ref[...])
        dh_ref[rows, :] += dot_nt(d_pre, w1)
        return carry

    lax.fori_loop(0, T // MLP_ROWS, rows_step, 0)

    def grad_step(i, carry):
        for side, out in ((1 - core, gw1_send), (core, gw1_keep)):
            rows = pl.ds(pl.multiple_of((2 * i + side) * 128, 128), 128)
            out[i] = dot(ht_ref[rows, :], dpre_s[...])
        rows = pl.ds(pl.multiple_of(i * 256, 256), 256)
        for side, out in ((1 - core, gw2_send), (core, gw2_keep)):
            out[0, rows, :] = dot(gt_ref[rows, :], act_s[:, pl.ds(pl.multiple_of(side * FC, FC), FC)])
        return carry

    lax.fori_loop(0, D // 256, grad_step, 0)


def mlp_chunk(h, g, ht, gt, weights, b1):
    cols = NS * FC
    once = pl.Buffered(1)
    whole = lambda shape: pl.BlockSpec(shape, lambda s: (0, 0), pipeline_mode=once)
    return pl.pallas_call(
        mlp_kernel,
        grid=(cols // BLK,),
        in_specs=[whole((T, D)), whole((T, D)), whole((D, T)), whole((D, T)),
                  pl.BlockSpec((NS, D // NS, BLK), lambda s: (0, 0, s)),
                  pl.BlockSpec((2, D // NS, cols), lambda s: (s, 1, 0)),
                  pl.BlockSpec((1, BLK), lambda s: (0, s))],
        out_specs=[whole((T, D)), whole((T, D)),
                   *[pl.BlockSpec((4, D // NS, BLK), lambda s: (0, 0, s))] * 2,
                   *[pl.BlockSpec((1, D, FC), lambda s: (s, 0, 0))] * 2,
                   pl.BlockSpec((1, BLK), lambda s: (0, s))],
        out_shape=[jax.ShapeDtypeStruct((T, D), F32), jax.ShapeDtypeStruct((T, D), F32),
                   *[jax.ShapeDtypeStruct((4, D // NS, cols), F32)] * 2, *[jax.ShapeDtypeStruct((4, D, FC), F32)] * 2,
                   jax.ShapeDtypeStruct((1, cols), F32)],
        scratch_shapes=[pltpu.VMEM((T, BLK), BF16), pltpu.VMEM((T, BLK), BF16), pltpu.VMEM((BLK, D), BF16)],
        compiler_params=pltpu.CompilerParams(dimension_semantics=("arbitrary",), vmem_limit_bytes=62 * 1024 * 1024),
        cost_estimate=pl.CostEstimate(flops=12 * T * D * cols, bytes_accessed=60_000_000, transcendentals=T * cols),
        name="mlp_fwd_bwd",
    )(h, g, ht, gt, weights, weights, b1)


POST_ROWS = 200


def post_kernel(m0_ref, m1_ref, d0_ref, d1_ref, x_ref, att_ref, g_ref, vec_ref, z_ref, res_ref, da_ref, sum_ref):
    row = lambda i: vec_ref[i:i + 1, :]
    att = att_ref[...]
    y = x_ref[...].astype(F32) + row(3) * att
    m = m0_ref[...] + m1_ref[...] + row(6)
    g = g_ref[...].astype(F32)
    z_ref[...] = (y + row(7) * m).astype(BF16)
    xhat, rstd = ln_stats(y)
    dh = d0_ref[...] + d1_ref[...]
    res = g + ln_back(xhat, rstd, dh * row(4))
    res_ref[...] = res
    da = res * row(3)
    da_ref[...] = da.astype(BF16)

    @pl.when(pl.program_id(0) == 0)
    def _():
        sum_ref[...] = jnp.zeros_like(sum_ref)

    for i, val in ((2, da), (3, res * att), (4, dh * xhat), (5, dh), (6, g * row(7)), (7, g * m)):
        sum_ref[i:i + 1, :] += jnp.sum(val, axis=0, keepdims=True)


def post_mlp(m0, m1, d0, d1, x, att, g, vec):
    rows = pl.BlockSpec((POST_ROWS, D), lambda i: (i, 0))
    fixed = pl.BlockSpec((8, D), lambda i: (0, 0))
    return pl.pallas_call(
        post_kernel,
        grid=(T // POST_ROWS,),
        in_specs=[rows] * 7 + [fixed],
        out_specs=[rows, rows, rows, fixed],
        out_shape=[jax.ShapeDtypeStruct((T, D), BF16), jax.ShapeDtypeStruct((T, D), F32), jax.ShapeDtypeStruct((T, D), BF16),
                   jax.ShapeDtypeStruct((8, D), F32)],
        compiler_params=pltpu.CompilerParams(dimension_semantics=("arbitrary",)),
        cost_estimate=pl.CostEstimate(flops=5_000_000_000, bytes_accessed=56_000_000, transcendentals=T),
        name="post_mlp",
    )(m0, m1, d0, d1, x, att, g, vec)


def ln_stats(t):
    mean = jnp.mean(t, axis=-1, keepdims=True)
    centered = t - mean
    variance = jnp.mean(centered * centered, axis=-1, keepdims=True)
    rstd = lax.rsqrt(variance + LN_EPS)
    return centered * rstd, rstd


def ln_back(xhat, rstd, d):
    return rstd * (d - jnp.mean(d, axis=-1, keepdims=True) - xhat * jnp.mean(d * xhat, axis=-1, keepdims=True))


LN1_ROWS = 400


def ln1_kernel(d0_ref, d1_ref, w_ref, x_ref, res_ref, vec_ref, dx_ref, sum_ref):
    dh = dot_nt(d0_ref[...], w_ref[:, :3 * HALF]) + dot_nt(d1_ref[...], w_ref[:, 3 * HALF:])
    xhat, rstd = ln_stats(x_ref[...].astype(F32))
    dx_ref[...] = (res_ref[...] + ln_back(xhat, rstd, dh * vec_ref[0:1, :])).astype(BF16)

    @pl.when(pl.program_id(0) == 0)
    def _():
        sum_ref[...] = jnp.zeros_like(sum_ref)

    sum_ref[0:1, :] += jnp.sum(dh * xhat, axis=0, keepdims=True)
    sum_ref[1:2, :] += jnp.sum(dh, axis=0, keepdims=True)


def ln1_backward(d0, d1, w_first, x, res, vec):
    rows = pl.BlockSpec((LN1_ROWS, D), lambda i: (i, 0))
    fixed = pl.BlockSpec((8, D), lambda i: (0, 0))
    return pl.pallas_call(
        ln1_kernel,
        grid=(T // LN1_ROWS,),
        in_specs=[pl.BlockSpec((LN1_ROWS, 3 * HALF), lambda i: (i, 0))] * 2
        + [pl.BlockSpec((D, 3 * D), lambda i: (0, 0), pipeline_mode=pl.Buffered(1)), rows, rows, fixed],
        out_specs=[rows, fixed],
        out_shape=[jax.ShapeDtypeStruct((T, D), BF16), jax.ShapeDtypeStruct((8, D), F32)],
        compiler_params=pltpu.CompilerParams(dimension_semantics=("arbitrary",)),
        cost_estimate=pl.CostEstimate(flops=6 * T * D * D, bytes_accessed=30_000_000, transcendentals=T),
        name="ln1_back",
    )(d0, d1, w_first, x, res, vec)


def gather_rows(shard):
    return lax.all_gather(shard, "fsdp", axis=0, tiled=True)


def exchange(val, bit):
    return lax.ppermute(val, "fsdp", [(i, i ^ bit) for i in range(NS)])


def pick(val, axis, index):
    return lax.dynamic_index_in_dim(val, index, axis, keepdims=False)


class Reduction:
    def __init__(self, send, keep, core, x_first, first=0):
        self.rows, self.cols = send.shape[2:]
        self.keep, self.core, self.x_first, self.first = keep, core, x_first, first
        self.near_bit, self.far_bit = (2, 4) if x_first else (4, 2)
        self.got1 = exchange(send, 1)

    def pick_yx(self, near, far):
        return (far, near) if self.x_first else (near, far)

    def term_specs(self, rows, near, far, at):
        def keep_map(s, idx):
            core = idx[2] if self.core else 0
            return (*self.pick_yx(near(s, idx), far(s, idx)), core, self.first // rows + at(s), 0)

        def got_map(s, idx):
            return (*self.pick_yx(near(s, idx), far(s, idx)), at(s), 0)

        return [(self.keep, pl.BlockSpec((None, None, None, rows, self.cols), keep_map)),
                (self.got1, pl.BlockSpec((None, None, rows, self.cols), got_map))]

    def plan(self, stage, n):
        mine = (lambda idx: idx[0], lambda idx: idx[1]) if self.x_first else (lambda idx: idx[1], lambda idx: idx[0])
        my_near, my_far = mine
        if stage == "near":
            per = n // 2
            rows = self.rows // per
            ins = self.term_specs(rows, lambda s, idx: 1 - my_near(idx), lambda s, idx: s // per, lambda s: s % per)
            return ins, (2, self.rows, self.cols), pl.BlockSpec((None, rows, self.cols), lambda s, idx: (s // per, s % per, 0))
        rows = self.rows // n
        far = (lambda s, idx: 1 - my_far(idx)) if stage == "far" else (lambda s, idx: my_far(idx))
        ins = self.term_specs(rows, lambda s, idx: my_near(idx), far, lambda s: s)
        ins.append((self.got2, pl.BlockSpec((None, rows, self.cols), lambda s, idx: (far(s, idx), s, 0))))
        flat = pl.BlockSpec((rows, self.cols), lambda s, idx: (s, 0))
        if stage == "rep":
            ins.append((self.got3, flat))
        return ins, (self.rows, self.cols), flat

    def start(self, stage, value):
        if stage == "near":
            self.got2 = exchange(value, self.near_bit)
        elif stage == "far":
            self.got3 = exchange(value, self.far_bit)
        else:
            self.part = value
            self.got4 = lax.ppermute(value, "rep", [(0, 1), (1, 0)])

    def result(self):
        return self.part + self.got4


def moves_kernel(counts, idx_ref, *refs):
    outs = refs[sum(counts):]
    at = 0
    for count, out in zip(counts, outs):
        total = refs[at][...]
        for ref in refs[at + 1:at + count]:
            total = total + ref[...]
        out[...] = total
        at += count


MOVE_STEPS = 4


def advance(anchor, *moves):
    flat = [(r, stage) for group, stage in moves for r in group]
    plans = [r.plan(stage, MOVE_STEPS) for r, stage in flat]
    me = lax.axis_index("fsdp")
    idx = jnp.stack([lax.rem(me // 2, 2), me // 4, lax.rem(me, 2)]).astype(jnp.int32)
    values = pl.pallas_call(
        functools.partial(moves_kernel, [len(ins) for ins, _, _ in plans]),
        grid_spec=pltpu.PrefetchScalarGridSpec(
            num_scalar_prefetch=1, grid=(MOVE_STEPS,),
            in_specs=[spec for ins, _, _ in plans for _, spec in ins],
            out_specs=[spec for _, _, spec in plans]),
        out_shape=[jax.ShapeDtypeStruct(shape, F32) for _, shape, _ in plans],
        compiler_params=pltpu.CompilerParams(dimension_semantics=("arbitrary",)),
        cost_estimate=pl.CostEstimate(flops=1_000_000_000, bytes_accessed=10_000_000, transcendentals=0),
        name="moves",
    )(idx, *[val for ins, _, _ in plans for val, _ in ins])
    anchor, values = lax.optimization_barrier((anchor, values))
    for (r, stage), value in zip(flat, values):
        r.start(stage, value)
    return anchor


def split_full(full, pieces):
    rows = full.shape[0] // NS
    parts = full.reshape(2, 2, 2, rows, full.shape[1])
    core = lax.rem(lax.axis_index("fsdp"), 2)
    cut = rows // pieces
    return [Reduction(pick(parts[:, :, :, i * cut:(i + 1) * cut], 2, 1 - core), parts, True, i % 2 == 0, i * cut)
            for i in range(pieces)]


def row_major(val):
    return with_layout_constraint(val, Layout(major_to_minor=tuple(range(val.ndim))))


def solution(mesh):
    batch_spec = P(("rep", "fsdp"), None, None)
    row_spec = P("fsdp", None)
    flat_spec = P("fsdp")
    col_spec = P(None, "fsdp")
    param_specs = (row_spec, flat_spec, row_spec, row_spec, flat_spec, row_spec, col_spec)

    def layer_step(x_loc, dz_loc, w_qkv, b_qkv, w_out, w_up, b_up, w_down, vec_params):
        def by_half(val):
            lead = val.shape[:-1]
            return val.reshape(lead + (3, 2, HALF)).swapaxes(-3, -2).reshape(lead + (3 * D,))

        def from_half(val):
            lead = val.shape[:-1]
            return val.reshape(lead + (2, 3, HALF)).swapaxes(-3, -2).reshape(lead + (3 * D,))

        w_first = row_major(jnp.concatenate([by_half(w_qkv.astype(BF16)), w_out.astype(BF16)], axis=1))
        w_first = row_major(gather_rows(w_first))
        wq = w_first[:, :3 * D]
        wo = w_first[:, 3 * D:]
        up_split = w_up.reshape(D // NS, NS, CHUNKS, FC)
        down_split = w_down.reshape(CHUNKS, 2, D // NS, D)
        w_mlp = []
        for c in range(CHUNKS):
            up = up_split[:, :, c].reshape(D // NS, NS * FC).astype(BF16)
            down = jnp.concatenate([down_split[c, 0], down_split[c, 1]], axis=1).astype(BF16)
            shard = row_major(jnp.concatenate([up, down], axis=0))
            w_mlp.append(row_major(lax.all_gather(shard, "fsdp", axis=0, tiled=False)))
        small = jnp.concatenate([b_qkv, b_up, vec_params.reshape(-1)]).astype(BF16)
        small = lax.all_gather(small, "fsdp", axis=0, tiled=False).astype(F32)
        nq, nu = b_qkv.shape[0], b_up.shape[0]
        bias_qkv = by_half(small[:, :nq].reshape(-1))
        bias_up = small[:, nq:nq + nu].reshape(NS, CHUNKS, FC)
        vec = small[:, nq + nu:].reshape(NS, 8, D // NS).transpose(1, 0, 2).reshape(8, D)
        ln1_gain, ln1_bias, out_bias, scale_attn, ln2_gain, ln2_bias, _, scale_mlp = vec

        x_flat = row_major(x_loc.reshape(T, D))
        g_flat = row_major(dz_loc.reshape(T, D))
        x = x_flat.astype(F32)
        d_mlp_bf = row_major((g_flat.astype(F32) * scale_mlp).astype(BF16))
        d_mlp_t = d_mlp_bf.T

        xhat1, _ = ln_stats(x)
        h1 = (xhat1 * ln1_gain + ln1_bias).astype(BF16)
        qkv = (dot(h1, wq) + bias_qkv).astype(BF16)
        heads = attn_forward(qkv)
        att = dot(heads, wo) + out_bias
        y = x + scale_attn * att
        xhat2, _ = ln_stats(y)
        h2 = row_major((xhat2 * ln2_gain + ln2_bias).astype(BF16))
        h2_t = h2.T

        quad = lambda v: v.reshape((2, 2) + v.shape[1:])
        five = lambda v: v.reshape((2, 2, 1) + v.shape[1:])
        partial = []
        grad_bup = []
        mlp = []
        for c in range(CHUNKS):
            m_c, dh_c, up_send, up_keep, down_send, down_keep, gb = mlp_chunk(
                h2, d_mlp_bf, h2_t, d_mlp_t, w_mlp[c], bias_up[:, c].reshape(1, -1))
            mlp.append([Reduction(quad(up_send), five(up_keep), False, True),
                        Reduction(quad(down_send), five(down_keep), False, False)])
            grad_bup.append(gb.reshape(NS, FC))
            partial += [m_c, dh_c]
        partial = advance(partial, (mlp[0], "near"))
        z, g_resid, d_att_bf, vec_sums = post_mlp(partial[0], partial[2], partial[1], partial[3], x_flat, att, g_flat, vec)
        d_heads = dot_nt(d_att_bf, wo).astype(BF16)
        out_red = split_full(dot_tn(heads, d_att_bf), 2)

        d_heads = advance(d_heads, (mlp[0], "far"), (mlp[1], "near"))
        d_qkv0, gb0 = attn_backward(qkv, d_heads, 0)
        qkv0 = split_full(dot_tn(h1, d_qkv0), 2)
        d_qkv0, z = lax.optimization_barrier((d_qkv0, z))
        z = row_major(z.reshape(SEQS, SEQ, D))
        z, d_heads = advance((z, d_heads), (out_red, "near"), (mlp[0], "rep"))
        d_heads = advance(d_heads, (mlp[1], "far"))
        d_qkv1, gb1 = attn_backward(qkv, d_heads, 1)
        gw1 = dot_tn(h1, d_qkv1)
        qkv1 = split_full(gw1, 2)
        d_qkv1 = advance(d_qkv1, (qkv0, "near"), (out_red, "far"), (mlp[1], "rep"))
        d_qkv1 = advance(d_qkv1, (qkv1, "near"))
        dx, ln1_sums = ln1_backward(d_qkv0, d_qkv1, w_first, x_flat, g_resid, vec)
        grad_vec = jnp.concatenate([ln1_sums[:2], vec_sums[2:]], axis=0)
        grad_bqkv = from_half(jnp.sum(jnp.concatenate([gb0, gb1], axis=2), axis=(0, 1))).reshape(NS, nq)
        grad_bup = jnp.stack(grad_bup, axis=1).reshape(NS, nu)
        grad_vec = grad_vec.reshape(8, NS, D // NS).transpose(1, 0, 2).reshape(NS, D)
        small_grads = jnp.concatenate([grad_bqkv, grad_bup, grad_vec, jnp.zeros((NS, 64 * 128 - nq - nu - D), F32)], axis=1)
        small_red = split_full(small_grads.reshape(NS * 64, 128), 1)
        dx = advance(dx, (qkv1, "far"), (qkv0, "far"), (out_red, "rep"))
        dx = row_major(dx.reshape(SEQS, SEQ, D))
        advance((), (qkv1, "rep"), (qkv0, "rep"), (small_red, "near"))
        advance((), (small_red, "far"))
        advance((), (small_red, "rep"))
        whole = lambda group: jnp.concatenate([r.result() for r in group], axis=0)
        grad_w_out = whole(out_red)
        grad_w_qkv = from_half(jnp.concatenate([whole(qkv0), whole(qkv1)], axis=1))
        grad_up = [pair[0].result().reshape(D // NS, NS, FC) for pair in mlp]
        grad_down = [pair[1].result().T for pair in mlp]

        mine = small_red[0].result().reshape(-1)
        return (z, dx, grad_w_qkv, mine[:nq], grad_w_out,
                jnp.stack(grad_up, axis=2).reshape(D // NS, FF), mine[nq:nq + nu],
                jnp.concatenate(grad_down, axis=0), mine[nq + nu:nq + nu + D].reshape(8, D // NS))

    return jax.shard_map(layer_step, mesh=mesh, in_specs=(batch_spec, batch_spec) + param_specs,
                         out_specs=(batch_spec, batch_spec) + param_specs, check_vma=False)
```

```python
import functools

import jax
import jax.numpy as jnp
from jax import lax
from jax.experimental import pallas as pl
from jax.experimental.layout import Layout, with_layout_constraint
from jax.experimental.pallas import tpu as pltpu
from jax.sharding import PartitionSpec as P


HEADS = 16
LN_EPS = 1e-5
SEQ = 50
D = 1024
FF = 4096
SEQS = 32
T = SEQS * SEQ
NS = 8
CHUNKS = 2
HALF = D // 2
FC = FF // NS // CHUNKS
GROUP = 8
ROWS = GROUP * SEQ
PAIR = 2 * SEQ
WIN = 112
SCALE = (D // HEADS) ** -0.5
NEG = -3.0e38
F32 = jnp.float32
BF16 = jnp.bfloat16

ERFC_P = 0.45
ERFC_Q = (0.25388532876968384, 0.25388315320014954, 0.22827185690402985, 0.1752501279115677, 0.11996052414178848,
          -0.0223874319344759, 0.14245237410068512, -0.30063509941101074, 0.19071702659130096, -0.041397832334041595)


def dot(a, b):
    return lax.dot_general(a, b, (((1,), (0,)), ((), ())), preferred_element_type=F32)


def dot_nt(a, b):
    return lax.dot_general(a, b, (((1,), (1,)), ((), ())), preferred_element_type=F32)


def dot_tn(a, b):
    return lax.dot_general(a, b, (((0,), (0,)), ((), ())), preferred_element_type=F32)


def gelu_and_slope(u):
    dens = jnp.exp(u * u * -0.5)
    t = 1.0 / (1.0 + (ERFC_P * 0.5 ** 0.5) * jnp.abs(u))
    q = jnp.full_like(t, ERFC_Q[-1])
    for coef in ERFC_Q[-2::-1]:
        q = q * t + coef
    half = (0.5 * dens) * (t * q)
    cdf = jnp.where(u > 0, 1.0 - half, half)
    return u * cdf, cdf + u * dens * 0.3989422804014327


def window_parts(j):
    start = 16 * ((PAIR * j) // 16)
    off = PAIR * j - start
    r = lax.broadcasted_iota(jnp.int32, (WIN, WIN), 0)
    c = lax.broadcasted_iota(jnp.int32, (WIN, WIN), 1)

    def seq_of(v):
        one = jnp.int32(1)
        zero = jnp.int32(0)
        return (jnp.where(v >= off, one, zero) + jnp.where(v >= off + SEQ, one, zero)
                + jnp.where(v >= off + PAIR, one, zero))

    bias = jnp.where(seq_of(r) == seq_of(c), 0.0, NEG)
    row = lax.broadcasted_iota(jnp.int32, (WIN, 128), 0)
    lane = lax.broadcasted_iota(jnp.int32, (WIN, 128), 1)
    inside = (row >= off) & (row < off + PAIR)
    return start, bias, inside, lane < 64


def softmax_rows(s, bias2):
    s = jnp.where(bias2 == 0.0, s, NEG)
    m = jnp.max(s, axis=1, keepdims=True)
    p = jnp.exp2((s - m) * (SCALE * 1.4426950408889634))
    return p * (1.0 / jnp.sum(p, axis=1, keepdims=True))


def attn_fwd_kernel(q_ref, k_ref, v_ref, o_ref):
    for j in range(ROWS // PAIR):
        start, bias, inside, even = window_parts(j)
        bias2 = jnp.concatenate([bias, bias], axis=0)
        m_even = jnp.where(even, 1.0, 0.0).astype(BF16)
        m_odd = jnp.where(even, 0.0, 1.0).astype(BF16)
        for hp in range(q_ref.shape[1] // 128):
            cols = slice(hp * 128, hp * 128 + 128)
            q = q_ref[start:start + WIN, cols]
            k = k_ref[start:start + WIN, cols]
            v = v_ref[start:start + WIN, cols]
            q2 = jnp.concatenate([q * m_even, q * m_odd], axis=0)
            p = softmax_rows(dot_nt(q2, k), bias2)
            o2 = dot(p.astype(BF16), v)
            o = jnp.where(inside, jnp.where(even, o2[:WIN], o2[WIN:]), 0.0).astype(BF16)
            if j:
                o_ref[start:start + 16, cols] += o[:16]
                o_ref[start + 16:start + WIN, cols] = o[16:]
            else:
                o_ref[start:start + WIN, cols] = o


def attn_bwd_kernel(q_ref, k_ref, v_ref, g_ref, d_ref, b_ref):
    parts = []
    for j in range(ROWS // PAIR):
        start, bias, inside, even = window_parts(j)
        one_even = jnp.where(even, 1.0, 0.0)
        parts.append((start, jnp.concatenate([bias, bias], axis=0), one_even.astype(BF16), (1.0 - one_even).astype(BF16),
                      jnp.where(inside, one_even, 0.0).astype(BF16), jnp.where(inside, 1.0 - one_even, 0.0).astype(BF16)))

    def head_pair(hp):
        cols = slice(hp * 128, hp * 128 + 128)
        sums = [jnp.zeros((1, 128), F32) for _ in range(3)]
        for j, (start, bias2, m_even, m_odd, g_even, g_odd) in enumerate(parts):
            q = q_ref[start:start + WIN, cols]
            k = k_ref[start:start + WIN, cols]
            v = v_ref[start:start + WIN, cols]
            g = g_ref[start:start + WIN, cols]
            q2 = jnp.concatenate([q * m_even, q * m_odd], axis=0)
            g2 = jnp.concatenate([g * g_even, g * g_odd], axis=0)
            p = softmax_rows(dot_nt(q2, k), bias2)
            dp = dot_nt(g2, v)
            ds = (p * (dp - jnp.sum(dp * p, axis=1, keepdims=True)) * SCALE).astype(BF16)
            dq2 = dot(ds, k)
            even = lax.broadcasted_iota(jnp.int32, (WIN, 128), 1) < 64
            dq = jnp.where(even, dq2[:WIN], dq2[WIN:])
            dk = dot_tn(ds, q2)
            dv = dot_tn(p.astype(BF16), g2)
            for i, val in enumerate((dq, dk, dv)):
                out = slice(hp * 128 + i * HALF, hp * 128 + i * HALF + 128)
                sums[i] = sums[i] + jnp.sum(val, axis=0, keepdims=True)
                val = val.astype(BF16)
                if j:
                    d_ref[start:start + 16, out] += val[:16]
                    d_ref[start + 16:start + WIN, out] = val[16:]
                else:
                    d_ref[start:start + WIN, out] = val
        for i in range(3):
            b_ref[0, :, hp * 128 + i * HALF:hp * 128 + i * HALF + 128] = sums[i]

    for hp in range(HALF // 128):
        head_pair(hp)


ATT_COLS = 256


def attn_forward(qkv):
    per = HALF // ATT_COLS
    spec = lambda part: pl.BlockSpec((ROWS, ATT_COLS), lambda g, c: (g, (c // per * 3 + part) * per + c % per))
    return pl.pallas_call(
        attn_fwd_kernel,
        grid=(T // ROWS, D // ATT_COLS),
        in_specs=[spec(0), spec(1), spec(2)],
        out_specs=pl.BlockSpec((ROWS, ATT_COLS), lambda g, c: (g, c)),
        out_shape=jax.ShapeDtypeStruct((T, D), BF16),
        compiler_params=pltpu.CompilerParams(dimension_semantics=("arbitrary", "arbitrary")),
        cost_estimate=pl.CostEstimate(flops=8_000_000_000, bytes_accessed=13_000_000, transcendentals=3_000_000),
        name="attn_fwd",
    )(qkv, qkv, qkv)


def attn_backward(qkv, d_heads, half):
    spec = lambda at: pl.BlockSpec((ROWS, HALF), lambda g: (g, at))
    return pl.pallas_call(
        attn_bwd_kernel,
        grid=(T // ROWS,),
        in_specs=[spec(3 * half), spec(3 * half + 1), spec(3 * half + 2), spec(half)],
        out_specs=[pl.BlockSpec((ROWS, 3 * HALF), lambda g: (g, 0)), pl.BlockSpec((1, 1, 3 * HALF), lambda g: (g, 0, 0))],
        out_shape=[jax.ShapeDtypeStruct((T, 3 * HALF), BF16), jax.ShapeDtypeStruct((T // ROWS, 1, 3 * HALF), F32)],
        compiler_params=pltpu.CompilerParams(dimension_semantics=("arbitrary",)),
        cost_estimate=pl.CostEstimate(flops=16_000_000_000, bytes_accessed=12_000_000, transcendentals=1_500_000),
        name="attn_bwd",
    )(qkv, qkv, qkv, d_heads)


MLP_ROWS = 800
BLK = 2 * FC


def mlp_kernel(h_ref, g_ref, ht_send, ht_keep, gt_ref, w1_ref, wd_ref, b1_ref, m_ref, dh_ref,
               gw1_send, gw1_keep, gw2_send, gw2_keep, gb_ref, act_s, dpre_s, w2_ref):
    step = pl.program_id(0)
    core = lax.rem(lax.axis_index("fsdp"), 2)
    gb_ref[...] = jnp.zeros_like(gb_ref)
    for n in range(4):
        w2_ref[n * 128:(n + 1) * 128, :] = wd_ref[n // 2, :, n % 2 * D:(n % 2 + 1) * D]

    @pl.when(step == 0)
    def _():
        m_ref[...] = jnp.zeros_like(m_ref)
        dh_ref[...] = jnp.zeros_like(dh_ref)

    def rows_step(i, carry):
        rows = pl.ds(pl.multiple_of(i * MLP_ROWS, 16), MLP_ROWS)
        w1 = w1_ref[...].reshape(D, BLK)
        u = dot(h_ref[rows, :], w1) + b1_ref[...]
        d_act = dot_nt(g_ref[rows, :], w2_ref[...])
        act, slope = gelu_and_slope(u)
        act = act.astype(BF16)
        d_pre = d_act * slope
        gb_ref[...] += jnp.sum(d_pre, axis=0, keepdims=True)
        d_pre = d_pre.astype(BF16)
        act_s[rows, :] = act
        dpre_s[rows, :] = d_pre
        m_ref[rows, :] += dot(act, w2_ref[...])
        dh_ref[rows, :] += dot_nt(d_pre, w1)
        return carry

    lax.fori_loop(0, T // MLP_ROWS, rows_step, 0)

    def grad_step(i, carry):
        for src, out in ((ht_send, gw1_send), (ht_keep, gw1_keep)):
            two = pl.ds(2 * i, 2)
            out[two] = dot(src[two].reshape(2 * D // NS, T), dpre_s[...]).reshape(2, D // NS, BLK)
        rows = pl.ds(pl.multiple_of(i * (D // 2), D // 2), D // 2)
        for side, out in ((1 - core, gw2_send), (core, gw2_keep)):
            out[0, rows, :] = dot(gt_ref[rows, :], act_s[:, pl.ds(pl.multiple_of(side * FC, FC), FC)])
        return carry

    lax.fori_loop(0, 2, grad_step, 0)


def mlp_chunk(h, g, ht, gt, weights, b1):
    cols = NS * FC
    once = pl.Buffered(1)
    whole = lambda shape: pl.BlockSpec(shape, lambda s: (0, 0), pipeline_mode=once)
    core = lambda: lax.rem(lax.axis_index("fsdp"), 2)
    half = lambda side: pl.BlockSpec((4, None, D // NS, T), lambda s: (0, side(), 0, 0), pipeline_mode=once)
    ht = ht.reshape(4, 2, D // NS, T)
    return pl.pallas_call(
        mlp_kernel,
        grid=(cols // BLK,),
        in_specs=[whole((T, D)), whole((T, D)), half(lambda: 1 - core()), half(core), whole((D, T)),
                  pl.BlockSpec((NS, D // NS, BLK), lambda s: (0, 0, s)),
                  pl.BlockSpec((2, D // NS, cols), lambda s: (s, 1, 0)),
                  pl.BlockSpec((1, BLK), lambda s: (0, s))],
        out_specs=[whole((T, D)), whole((T, D)),
                   *[pl.BlockSpec((4, D // NS, BLK), lambda s: (0, 0, s))] * 2,
                   *[pl.BlockSpec((1, D, FC), lambda s: (s, 0, 0))] * 2,
                   pl.BlockSpec((1, BLK), lambda s: (0, s))],
        out_shape=[jax.ShapeDtypeStruct((T, D), F32), jax.ShapeDtypeStruct((T, D), F32),
                   *[jax.ShapeDtypeStruct((4, D // NS, cols), F32)] * 2, *[jax.ShapeDtypeStruct((4, D, FC), F32)] * 2,
                   jax.ShapeDtypeStruct((1, cols), F32)],
        scratch_shapes=[pltpu.VMEM((T, BLK), BF16), pltpu.VMEM((T, BLK), BF16), pltpu.VMEM((BLK, D), BF16)],
        compiler_params=pltpu.CompilerParams(dimension_semantics=("arbitrary",), vmem_limit_bytes=62 * 1024 * 1024),
        cost_estimate=pl.CostEstimate(flops=12 * T * D * cols, bytes_accessed=60_000_000, transcendentals=T * cols),
        name="mlp_fwd_bwd",
    )(h, g, ht, ht, gt, weights, weights, b1)


POST_ROWS = 200


def post_kernel(m0_ref, m1_ref, d0_ref, d1_ref, x_ref, att_ref, g_ref, vec_ref, z_ref, res_ref, da_ref, sum_ref):
    row = lambda i: vec_ref[i:i + 1, :]
    att = att_ref[...]
    y = x_ref[...].astype(F32) + row(3) * att
    m = m0_ref[...] + m1_ref[...] + row(6)
    g = g_ref[...].astype(F32)
    z_ref[...] = (y + row(7) * m).astype(BF16)
    xhat, rstd = ln_stats(y)
    dh = d0_ref[...] + d1_ref[...]
    res = g + ln_back(xhat, rstd, dh * row(4))
    res_ref[...] = res
    da = res * row(3)
    da_ref[...] = da.astype(BF16)

    @pl.when(pl.program_id(0) == 0)
    def _():
        sum_ref[...] = jnp.zeros_like(sum_ref)

    for i, val in ((2, da), (3, res * att), (4, dh * xhat), (5, dh), (6, g * row(7)), (7, g * m)):
        sum_ref[i:i + 1, :] += jnp.sum(val, axis=0, keepdims=True)


def post_mlp(m0, m1, d0, d1, x, att, g, vec):
    rows = pl.BlockSpec((POST_ROWS, D), lambda i: (i, 0))
    fixed = pl.BlockSpec((8, D), lambda i: (0, 0))
    return pl.pallas_call(
        post_kernel,
        grid=(T // POST_ROWS,),
        in_specs=[rows] * 7 + [fixed],
        out_specs=[rows, rows, rows, fixed],
        out_shape=[jax.ShapeDtypeStruct((T, D), BF16), jax.ShapeDtypeStruct((T, D), F32), jax.ShapeDtypeStruct((T, D), BF16),
                   jax.ShapeDtypeStruct((8, D), F32)],
        compiler_params=pltpu.CompilerParams(dimension_semantics=("arbitrary",)),
        cost_estimate=pl.CostEstimate(flops=5_000_000_000, bytes_accessed=56_000_000, transcendentals=T),
        name="post_mlp",
    )(m0, m1, d0, d1, x, att, g, vec)


def ln_stats(t):
    mean = jnp.mean(t, axis=-1, keepdims=True)
    centered = t - mean
    variance = jnp.mean(centered * centered, axis=-1, keepdims=True)
    rstd = lax.rsqrt(variance + LN_EPS)
    return centered * rstd, rstd


def ln_back(xhat, rstd, d):
    return rstd * (d - jnp.mean(d, axis=-1, keepdims=True) - xhat * jnp.mean(d * xhat, axis=-1, keepdims=True))


LN1_ROWS = 400


def ln1_kernel(d0_ref, d1_ref, w_ref, x_ref, res_ref, vec_ref, dx_ref, sum_ref):
    dh = dot_nt(d0_ref[...], w_ref[:, :3 * HALF]) + dot_nt(d1_ref[...], w_ref[:, 3 * HALF:])
    xhat, rstd = ln_stats(x_ref[...].astype(F32))
    dx_ref[...] = (res_ref[...] + ln_back(xhat, rstd, dh * vec_ref[0:1, :])).astype(BF16)

    @pl.when(pl.program_id(0) == 0)
    def _():
        sum_ref[...] = jnp.zeros_like(sum_ref)

    sum_ref[0:1, :] += jnp.sum(dh * xhat, axis=0, keepdims=True)
    sum_ref[1:2, :] += jnp.sum(dh, axis=0, keepdims=True)


def ln1_backward(d0, d1, w_first, x, res, vec):
    rows = pl.BlockSpec((LN1_ROWS, D), lambda i: (i, 0))
    fixed = pl.BlockSpec((8, D), lambda i: (0, 0))
    return pl.pallas_call(
        ln1_kernel,
        grid=(T // LN1_ROWS,),
        in_specs=[pl.BlockSpec((LN1_ROWS, 3 * HALF), lambda i: (i, 0))] * 2
        + [pl.BlockSpec((D, 3 * D), lambda i: (0, 0), pipeline_mode=pl.Buffered(1)), rows, rows, fixed],
        out_specs=[rows, fixed],
        out_shape=[jax.ShapeDtypeStruct((T, D), BF16), jax.ShapeDtypeStruct((8, D), F32)],
        compiler_params=pltpu.CompilerParams(dimension_semantics=("arbitrary",)),
        cost_estimate=pl.CostEstimate(flops=6 * T * D * D, bytes_accessed=30_000_000, transcendentals=T),
        name="ln1_back",
    )(d0, d1, w_first, x, res, vec)


def gather_rows(shard):
    return lax.all_gather(shard, "fsdp", axis=0, tiled=True)


def exchange(val, bit):
    return lax.ppermute(val, "fsdp", [(i, i ^ bit) for i in range(NS)])


def pick(val, axis, index):
    return lax.dynamic_index_in_dim(val, index, axis, keepdims=False)


class Reduction:
    def __init__(self, send, keep, core, x_first, first=0):
        self.rows, self.cols = send.shape[2:]
        self.keep, self.core, self.x_first, self.first = keep, core, x_first, first
        self.near_bit, self.far_bit = (2, 4) if x_first else (4, 2)
        self.got1 = exchange(send, 1)

    def pick_yx(self, near, far):
        return (far, near) if self.x_first else (near, far)

    def term_specs(self, rows, near, far, at):
        def keep_map(s, idx):
            core = idx[2] if self.core else 0
            return (*self.pick_yx(near(s, idx), far(s, idx)), core, self.first // rows + at(s), 0)

        def got_map(s, idx):
            return (*self.pick_yx(near(s, idx), far(s, idx)), at(s), 0)

        return [(self.keep, pl.BlockSpec((None, None, None, rows, self.cols), keep_map)),
                (self.got1, pl.BlockSpec((None, None, rows, self.cols), got_map))]

    def plan(self, stage, n):
        mine = (lambda idx: idx[0], lambda idx: idx[1]) if self.x_first else (lambda idx: idx[1], lambda idx: idx[0])
        my_near, my_far = mine
        if stage == "near":
            per = n // 2
            rows = self.rows // per
            ins = self.term_specs(rows, lambda s, idx: 1 - my_near(idx), lambda s, idx: s // per, lambda s: s % per)
            return ins, (2, self.rows, self.cols), pl.BlockSpec((None, rows, self.cols), lambda s, idx: (s // per, s % per, 0))
        rows = self.rows // n
        far = (lambda s, idx: 1 - my_far(idx)) if stage == "far" else (lambda s, idx: my_far(idx))
        ins = self.term_specs(rows, lambda s, idx: my_near(idx), far, lambda s: s)
        ins.append((self.got2, pl.BlockSpec((None, rows, self.cols), lambda s, idx: (far(s, idx), s, 0))))
        flat = pl.BlockSpec((rows, self.cols), lambda s, idx: (s, 0))
        if stage == "rep":
            ins.append((self.got3, flat))
        return ins, (self.rows, self.cols), flat

    def start(self, stage, value):
        if stage == "near":
            self.got2 = exchange(value, self.near_bit)
        elif stage == "far":
            self.got3 = exchange(value, self.far_bit)
        else:
            self.part = value
            self.got4 = lax.ppermute(value, "rep", [(0, 1), (1, 0)])

    def result(self):
        return self.part + self.got4


def moves_kernel(counts, idx_ref, *refs):
    outs = refs[sum(counts):]
    at = 0
    for count, out in zip(counts, outs):
        total = refs[at][...]
        for ref in refs[at + 1:at + count]:
            total = total + ref[...]
        out[...] = total
        at += count


MOVE_STEPS = 4


def advance(anchor, *moves):
    flat = [(r, stage) for group, stage in moves for r in group]
    plans = [r.plan(stage, MOVE_STEPS) for r, stage in flat]
    me = lax.axis_index("fsdp")
    idx = jnp.stack([lax.rem(me // 2, 2), me // 4, lax.rem(me, 2)]).astype(jnp.int32)
    values = pl.pallas_call(
        functools.partial(moves_kernel, [len(ins) for ins, _, _ in plans]),
        grid_spec=pltpu.PrefetchScalarGridSpec(
            num_scalar_prefetch=1, grid=(MOVE_STEPS,),
            in_specs=[spec for ins, _, _ in plans for _, spec in ins],
            out_specs=[spec for _, _, spec in plans]),
        out_shape=[jax.ShapeDtypeStruct(shape, F32) for _, shape, _ in plans],
        compiler_params=pltpu.CompilerParams(dimension_semantics=("arbitrary",)),
        cost_estimate=pl.CostEstimate(flops=1_000_000_000, bytes_accessed=10_000_000, transcendentals=0),
        name="moves",
    )(idx, *[val for ins, _, _ in plans for val, _ in ins])
    anchor, values = lax.optimization_barrier((anchor, values))
    for (r, stage), value in zip(flat, values):
        r.start(stage, value)
    return anchor


def split_full(full, pieces):
    rows = full.shape[0] // NS
    parts = full.reshape(2, 2, 2, rows, full.shape[1])
    core = lax.rem(lax.axis_index("fsdp"), 2)
    cut = rows // pieces
    return [Reduction(pick(parts[:, :, :, i * cut:(i + 1) * cut], 2, 1 - core), parts, True, i % 2 == 0, i * cut)
            for i in range(pieces)]


def row_major(val):
    return with_layout_constraint(val, Layout(major_to_minor=tuple(range(val.ndim))))


def solution(mesh):
    batch_spec = P(("rep", "fsdp"), None, None)
    row_spec = P("fsdp", None)
    flat_spec = P("fsdp")
    col_spec = P(None, "fsdp")
    param_specs = (row_spec, flat_spec, row_spec, row_spec, flat_spec, row_spec, col_spec)

    def layer_step(x_loc, dz_loc, w_qkv, b_qkv, w_out, w_up, b_up, w_down, vec_params):
        def by_half(val):
            lead = val.shape[:-1]
            return val.reshape(lead + (3, 2, HALF)).swapaxes(-3, -2).reshape(lead + (3 * D,))

        def from_half(val):
            lead = val.shape[:-1]
            return val.reshape(lead + (2, 3, HALF)).swapaxes(-3, -2).reshape(lead + (3 * D,))

        w_first = row_major(jnp.concatenate([by_half(w_qkv.astype(BF16)), w_out.astype(BF16)], axis=1))
        w_first = row_major(gather_rows(w_first))
        wq = w_first[:, :3 * D]
        wo = w_first[:, 3 * D:]
        up_split = w_up.reshape(D // NS, NS, CHUNKS, FC)
        down_split = w_down.reshape(CHUNKS, 2, D // NS, D)
        w_mlp = []
        for c in range(CHUNKS):
            up = up_split[:, :, c].reshape(D // NS, NS * FC).astype(BF16)
            down = jnp.concatenate([down_split[c, 0], down_split[c, 1]], axis=1).astype(BF16)
            shard = row_major(jnp.concatenate([up, down], axis=0))
            w_mlp.append(row_major(lax.all_gather(shard, "fsdp", axis=0, tiled=False)))
        small = jnp.concatenate([b_qkv, b_up, vec_params.reshape(-1)]).astype(BF16)
        small = lax.all_gather(small, "fsdp", axis=0, tiled=False).astype(F32)
        nq, nu = b_qkv.shape[0], b_up.shape[0]
        bias_qkv = by_half(small[:, :nq].reshape(-1))
        bias_up = small[:, nq:nq + nu].reshape(NS, CHUNKS, FC)
        vec = small[:, nq + nu:].reshape(NS, 8, D // NS).transpose(1, 0, 2).reshape(8, D)
        ln1_gain, ln1_bias, out_bias, scale_attn, ln2_gain, ln2_bias, _, scale_mlp = vec

        x_flat = row_major(x_loc.reshape(T, D))
        g_flat = row_major(dz_loc.reshape(T, D))
        x = x_flat.astype(F32)
        d_mlp_bf = row_major((g_flat.astype(F32) * scale_mlp).astype(BF16))
        d_mlp_t = d_mlp_bf.T

        xhat1, _ = ln_stats(x)
        h1 = (xhat1 * ln1_gain + ln1_bias).astype(BF16)
        qkv = (dot(h1, wq) + bias_qkv).astype(BF16)
        heads = attn_forward(qkv)
        att = dot(heads, wo) + out_bias
        y = x + scale_attn * att
        xhat2, _ = ln_stats(y)
        h2 = row_major((xhat2 * ln2_gain + ln2_bias).astype(BF16))
        h2_t = h2.T

        quad = lambda v: v.reshape((2, 2) + v.shape[1:])
        five = lambda v: v.reshape((2, 2, 1) + v.shape[1:])
        partial = []
        grad_bup = []
        mlp = []
        for c in range(CHUNKS):
            m_c, dh_c, up_send, up_keep, down_send, down_keep, gb = mlp_chunk(
                h2, d_mlp_bf, h2_t, d_mlp_t, w_mlp[c], bias_up[:, c].reshape(1, -1))
            mlp.append([Reduction(quad(up_send), five(up_keep), False, True),
                        Reduction(quad(down_send), five(down_keep), False, False)])
            grad_bup.append(gb.reshape(NS, FC))
            partial += [m_c, dh_c]
        partial = advance(partial, (mlp[0], "near"))
        z, g_resid, d_att_bf, vec_sums = post_mlp(partial[0], partial[2], partial[1], partial[3], x_flat, att, g_flat, vec)
        z = row_major(z.reshape(SEQS, SEQ, D))
        d_heads = dot_nt(d_att_bf, wo).astype(BF16)
        out_red = split_full(dot_tn(heads, d_att_bf), 2)

        d_heads = advance(d_heads, (mlp[0], "far"), (mlp[1], "near"))
        d_qkv0, gb0 = attn_backward(qkv, d_heads, 0)
        qkv0 = split_full(dot_tn(h1, d_qkv0), 2)
        d_heads = advance(d_heads, (out_red, "near"), (mlp[0], "rep"))
        d_heads = advance(d_heads, (mlp[1], "far"), (qkv0, "near"))
        d_qkv1, gb1 = attn_backward(qkv, d_heads, 1)
        gw1 = dot_tn(h1, d_qkv1)
        qkv1 = split_full(gw1, 2)
        d_qkv1 = advance(d_qkv1, (qkv0, "far"), (out_red, "far"), (mlp[1], "rep"))
        d_qkv1 = advance(d_qkv1, (qkv1, "near"))
        dx, ln1_sums = ln1_backward(d_qkv0, d_qkv1, w_first, x_flat, g_resid, vec)
        done = [(r.part, r.got4) for r in mlp[0]]
        dx, z, done = lax.optimization_barrier((dx, z, done))
        for r, (r.part, r.got4) in zip(mlp[0], done):
            pass
        grad_vec = jnp.concatenate([ln1_sums[:2], vec_sums[2:]], axis=0)
        grad_bqkv = from_half(jnp.sum(jnp.concatenate([gb0, gb1], axis=2), axis=(0, 1))).reshape(NS, nq)
        grad_bup = jnp.stack(grad_bup, axis=1).reshape(NS, nu)
        grad_vec = grad_vec.reshape(8, NS, D // NS).transpose(1, 0, 2).reshape(NS, D)
        small_grads = jnp.concatenate([grad_bqkv, grad_bup, grad_vec, jnp.zeros((NS, 64 * 128 - nq - nu - D), F32)], axis=1)
        small_red = split_full(small_grads.reshape(NS * 64, 128), 1)
        dx = advance(dx, (qkv1, "far"), (out_red, "rep"), (qkv0, "rep"))
        dx = row_major(dx.reshape(SEQS, SEQ, D))
        advance((), (qkv1, "rep"), (small_red, "near"))
        advance((), (small_red, "far"))
        advance((), (small_red, "rep"))
        whole = lambda group: jnp.concatenate([r.result() for r in group], axis=0)
        grad_w_out = whole(out_red)
        grad_w_qkv = from_half(jnp.concatenate([whole(qkv0), whole(qkv1)], axis=1))
        grad_up = [pair[0].result().reshape(D // NS, NS, FC) for pair in mlp]
        grad_down = [pair[1].result().T for pair in mlp]

        mine = small_red[0].result().reshape(-1)
        return (z, dx, grad_w_qkv, mine[:nq], grad_w_out,
                jnp.stack(grad_up, axis=2).reshape(D // NS, FF), mine[nq:nq + nu],
                jnp.concatenate(grad_down, axis=0), mine[nq + nu:nq + nu + D].reshape(8, D // NS))

    return jax.shard_map(layer_step, mesh=mesh, in_specs=(batch_spec, batch_spec) + param_specs,
                         out_specs=(batch_spec, batch_spec) + param_specs, check_vma=False)
```

```python
import functools

import jax
import jax.numpy as jnp
from jax import lax
from jax.experimental import pallas as pl
from jax.experimental.layout import Layout, with_layout_constraint
from jax.experimental.pallas import tpu as pltpu
from jax.sharding import PartitionSpec as P


HEADS = 16
LN_EPS = 1e-5
SEQ = 50
D = 1024
FF = 4096
SEQS = 32
T = SEQS * SEQ
NS = 8
CHUNKS = 2
HALF = D // 2
FC = FF // NS // CHUNKS
GROUP = 8
ROWS = GROUP * SEQ
PAIR = 2 * SEQ
WIN = 112
SCALE = (D // HEADS) ** -0.5
NEG = -3.0e38
F32 = jnp.float32
BF16 = jnp.bfloat16

ERFC_P = 0.45
ERFC_Q = (0.25388532876968384, 0.25388315320014954, 0.22827185690402985, 0.1752501279115677, 0.11996052414178848,
          -0.0223874319344759, 0.14245237410068512, -0.30063509941101074, 0.19071702659130096, -0.041397832334041595)


def dot(a, b):
    return lax.dot_general(a, b, (((1,), (0,)), ((), ())), preferred_element_type=F32)


def dot_nt(a, b):
    return lax.dot_general(a, b, (((1,), (1,)), ((), ())), preferred_element_type=F32)


def dot_tn(a, b):
    return lax.dot_general(a, b, (((0,), (0,)), ((), ())), preferred_element_type=F32)


def gelu_and_slope(u):
    dens = jnp.exp(u * u * -0.5)
    t = 1.0 / (1.0 + (ERFC_P * 0.5 ** 0.5) * jnp.abs(u))
    q = jnp.full_like(t, ERFC_Q[-1])
    for coef in ERFC_Q[-2::-1]:
        q = q * t + coef
    half = (0.5 * dens) * (t * q)
    cdf = jnp.where(u > 0, 1.0 - half, half)
    return u * cdf, cdf + u * dens * 0.3989422804014327


def window_parts(j):
    start = 16 * ((PAIR * j) // 16)
    off = PAIR * j - start
    r = lax.broadcasted_iota(jnp.int32, (WIN, WIN), 0)
    c = lax.broadcasted_iota(jnp.int32, (WIN, WIN), 1)

    def seq_of(v):
        one = jnp.int32(1)
        zero = jnp.int32(0)
        return (jnp.where(v >= off, one, zero) + jnp.where(v >= off + SEQ, one, zero)
                + jnp.where(v >= off + PAIR, one, zero))

    bias = jnp.where(seq_of(r) == seq_of(c), 0.0, NEG)
    row = lax.broadcasted_iota(jnp.int32, (WIN, 128), 0)
    lane = lax.broadcasted_iota(jnp.int32, (WIN, 128), 1)
    inside = (row >= off) & (row < off + PAIR)
    return start, bias, inside, lane < 64


def softmax_rows(s, bias2):
    s = jnp.where(bias2 == 0.0, s, NEG)
    m = jnp.max(s, axis=1, keepdims=True)
    p = jnp.exp2((s - m) * (SCALE * 1.4426950408889634))
    return p * (1.0 / jnp.sum(p, axis=1, keepdims=True))


def attn_fwd_kernel(q_ref, k_ref, v_ref, o_ref):
    for j in range(ROWS // PAIR):
        start, bias, inside, even = window_parts(j)
        bias2 = jnp.concatenate([bias, bias], axis=0)
        m_even = jnp.where(even, 1.0, 0.0).astype(BF16)
        m_odd = jnp.where(even, 0.0, 1.0).astype(BF16)
        for hp in range(q_ref.shape[1] // 128):
            cols = slice(hp * 128, hp * 128 + 128)
            q = q_ref[start:start + WIN, cols]
            k = k_ref[start:start + WIN, cols]
            v = v_ref[start:start + WIN, cols]
            q2 = jnp.concatenate([q * m_even, q * m_odd], axis=0)
            p = softmax_rows(dot_nt(q2, k), bias2)
            o2 = dot(p.astype(BF16), v)
            o = jnp.where(inside, jnp.where(even, o2[:WIN], o2[WIN:]), 0.0).astype(BF16)
            if j:
                o_ref[start:start + 16, cols] += o[:16]
                o_ref[start + 16:start + WIN, cols] = o[16:]
            else:
                o_ref[start:start + WIN, cols] = o


def attn_bwd_kernel(q_ref, k_ref, v_ref, g_ref, d_ref, b_ref):
    parts = []
    for j in range(ROWS // PAIR):
        start, bias, inside, even = window_parts(j)
        one_even = jnp.where(even, 1.0, 0.0)
        parts.append((start, jnp.concatenate([bias, bias], axis=0), one_even.astype(BF16), (1.0 - one_even).astype(BF16),
                      jnp.where(inside, one_even, 0.0).astype(BF16), jnp.where(inside, 1.0 - one_even, 0.0).astype(BF16)))

    def head_pair(hp):
        cols = slice(hp * 128, hp * 128 + 128)
        sums = [jnp.zeros((1, 128), F32) for _ in range(3)]
        for j, (start, bias2, m_even, m_odd, g_even, g_odd) in enumerate(parts):
            q = q_ref[start:start + WIN, cols]
            k = k_ref[start:start + WIN, cols]
            v = v_ref[start:start + WIN, cols]
            g = g_ref[start:start + WIN, cols]
            q2 = jnp.concatenate([q * m_even, q * m_odd], axis=0)
            g2 = jnp.concatenate([g * g_even, g * g_odd], axis=0)
            p = softmax_rows(dot_nt(q2, k), bias2)
            dp = dot_nt(g2, v)
            ds = (p * (dp - jnp.sum(dp * p, axis=1, keepdims=True)) * SCALE).astype(BF16)
            dq2 = dot(ds, k)
            even = lax.broadcasted_iota(jnp.int32, (WIN, 128), 1) < 64
            dq = jnp.where(even, dq2[:WIN], dq2[WIN:])
            dk = dot_tn(ds, q2)
            dv = dot_tn(p.astype(BF16), g2)
            for i, val in enumerate((dq, dk, dv)):
                out = slice(hp * 128 + i * HALF, hp * 128 + i * HALF + 128)
                sums[i] = sums[i] + jnp.sum(val, axis=0, keepdims=True)
                val = val.astype(BF16)
                if j:
                    d_ref[start:start + 16, out] += val[:16]
                    d_ref[start + 16:start + WIN, out] = val[16:]
                else:
                    d_ref[start:start + WIN, out] = val
        for i in range(3):
            b_ref[0, :, hp * 128 + i * HALF:hp * 128 + i * HALF + 128] = sums[i]

    for hp in range(HALF // 128):
        head_pair(hp)


ATT_COLS = 256


def attn_forward(qkv):
    per = HALF // ATT_COLS
    spec = lambda part: pl.BlockSpec((ROWS, ATT_COLS), lambda g, c: (g, (c // per * 3 + part) * per + c % per))
    return pl.pallas_call(
        attn_fwd_kernel,
        grid=(T // ROWS, D // ATT_COLS),
        in_specs=[spec(0), spec(1), spec(2)],
        out_specs=pl.BlockSpec((ROWS, ATT_COLS), lambda g, c: (g, c)),
        out_shape=jax.ShapeDtypeStruct((T, D), BF16),
        compiler_params=pltpu.CompilerParams(dimension_semantics=("arbitrary", "arbitrary")),
        cost_estimate=pl.CostEstimate(flops=8_000_000_000, bytes_accessed=13_000_000, transcendentals=3_000_000),
        name="attn_fwd",
    )(qkv, qkv, qkv)


def attn_backward(qkv, d_heads, half):
    spec = lambda at: pl.BlockSpec((ROWS, HALF), lambda g: (g, at))
    return pl.pallas_call(
        attn_bwd_kernel,
        grid=(T // ROWS,),
        in_specs=[spec(3 * half), spec(3 * half + 1), spec(3 * half + 2), spec(half)],
        out_specs=[pl.BlockSpec((ROWS, 3 * HALF), lambda g: (g, 0)), pl.BlockSpec((1, 1, 3 * HALF), lambda g: (g, 0, 0))],
        out_shape=[jax.ShapeDtypeStruct((T, 3 * HALF), BF16), jax.ShapeDtypeStruct((T // ROWS, 1, 3 * HALF), F32)],
        compiler_params=pltpu.CompilerParams(dimension_semantics=("arbitrary",)),
        cost_estimate=pl.CostEstimate(flops=16_000_000_000, bytes_accessed=12_000_000, transcendentals=1_500_000),
        name="attn_bwd",
    )(qkv, qkv, qkv, d_heads)


MLP_ROWS = 800
BLK = 2 * FC


def mlp_kernel(h_ref, g_ref, ht_send, ht_keep, gt_ref, w1_ref, wd_ref, b1_ref, m_ref, dh_ref,
               gw1_send, gw1_keep, gw2_send, gw2_keep, gb_ref, act_s, dpre_s, w2_ref):
    step = pl.program_id(0)
    core = lax.rem(lax.axis_index("fsdp"), 2)
    gb_ref[...] = jnp.zeros_like(gb_ref)
    for n in range(4):
        w2_ref[n * 128:(n + 1) * 128, :] = wd_ref[n // 2, :, n % 2 * D:(n % 2 + 1) * D]

    @pl.when(step == 0)
    def _():
        m_ref[...] = jnp.zeros_like(m_ref)
        dh_ref[...] = jnp.zeros_like(dh_ref)

    def rows_step(i, carry):
        rows = pl.ds(pl.multiple_of(i * MLP_ROWS, 16), MLP_ROWS)
        w1 = w1_ref[...].reshape(D, BLK)
        u = dot(h_ref[rows, :], w1) + b1_ref[...]
        d_act = dot_nt(g_ref[rows, :], w2_ref[...])
        act, slope = gelu_and_slope(u)
        act = act.astype(BF16)
        d_pre = d_act * slope
        gb_ref[...] += jnp.sum(d_pre, axis=0, keepdims=True)
        d_pre = d_pre.astype(BF16)
        act_s[rows, :] = act
        dpre_s[rows, :] = d_pre
        m_ref[rows, :] += dot(act, w2_ref[...])
        dh_ref[rows, :] += dot_nt(d_pre, w1)
        return carry

    lax.fori_loop(0, T // MLP_ROWS, rows_step, 0)

    def grad_step(i, carry):
        for src, out in ((ht_send, gw1_send), (ht_keep, gw1_keep)):
            two = pl.ds(2 * i, 2)
            out[two] = dot(src[two].reshape(2 * D // NS, T), dpre_s[...]).reshape(2, D // NS, BLK)
        rows = pl.ds(pl.multiple_of(i * (D // 2), D // 2), D // 2)
        for side, out in ((1 - core, gw2_send), (core, gw2_keep)):
            out[0, rows, :] = dot(gt_ref[rows, :], act_s[:, pl.ds(pl.multiple_of(side * FC, FC), FC)])
        return carry

    lax.fori_loop(0, 2, grad_step, 0)


def mlp_chunk(h, g, ht, gt, weights, b1):
    cols = NS * FC
    once = pl.Buffered(1)
    whole = lambda shape: pl.BlockSpec(shape, lambda s: (0, 0), pipeline_mode=once)
    core = lambda: lax.rem(lax.axis_index("fsdp"), 2)
    half = lambda side: pl.BlockSpec((4, None, D // NS, T), lambda s: (0, side(), 0, 0), pipeline_mode=once)
    ht = ht.reshape(4, 2, D // NS, T)
    return pl.pallas_call(
        mlp_kernel,
        grid=(cols // BLK,),
        in_specs=[whole((T, D)), whole((T, D)), half(lambda: 1 - core()), half(core), whole((D, T)),
                  pl.BlockSpec((NS, D // NS, BLK), lambda s: (0, 0, s)),
                  pl.BlockSpec((2, D // NS, cols), lambda s: (s, 1, 0)),
                  pl.BlockSpec((1, BLK), lambda s: (0, s))],
        out_specs=[whole((T, D)), whole((T, D)),
                   *[pl.BlockSpec((4, D // NS, BLK), lambda s: (0, 0, s))] * 2,
                   *[pl.BlockSpec((1, D, FC), lambda s: (s, 0, 0))] * 2,
                   pl.BlockSpec((1, BLK), lambda s: (0, s))],
        out_shape=[jax.ShapeDtypeStruct((T, D), F32), jax.ShapeDtypeStruct((T, D), F32),
                   *[jax.ShapeDtypeStruct((4, D // NS, cols), F32)] * 2, *[jax.ShapeDtypeStruct((4, D, FC), F32)] * 2,
                   jax.ShapeDtypeStruct((1, cols), F32)],
        scratch_shapes=[pltpu.VMEM((T, BLK), BF16), pltpu.VMEM((T, BLK), BF16), pltpu.VMEM((BLK, D), BF16)],
        compiler_params=pltpu.CompilerParams(dimension_semantics=("arbitrary",), vmem_limit_bytes=62 * 1024 * 1024),
        cost_estimate=pl.CostEstimate(flops=12 * T * D * cols, bytes_accessed=60_000_000, transcendentals=T * cols),
        name="mlp_fwd_bwd",
    )(h, g, ht, ht, gt, weights, weights, b1)


POST_ROWS = 200


def post_kernel(m0_ref, m1_ref, d0_ref, d1_ref, x_ref, att_ref, g_ref, vec_ref, z_ref, res_ref, da_ref, sum_ref):
    row = lambda i: vec_ref[i:i + 1, :]
    att = att_ref[...]
    y = x_ref[...].astype(F32) + row(3) * att
    m = m0_ref[...] + m1_ref[...] + row(6)
    g = g_ref[...].astype(F32)
    z_ref[...] = (y + row(7) * m).astype(BF16)
    xhat, rstd = ln_stats(y)
    dh = d0_ref[...] + d1_ref[...]
    res = g + ln_back(xhat, rstd, dh * row(4))
    res_ref[...] = res
    da = res * row(3)
    da_ref[...] = da.astype(BF16)

    @pl.when(pl.program_id(0) == 0)
    def _():
        sum_ref[...] = jnp.zeros_like(sum_ref)

    for i, val in ((2, da), (3, res * att), (4, dh * xhat), (5, dh), (6, g * row(7)), (7, g * m)):
        sum_ref[i:i + 1, :] += jnp.sum(val, axis=0, keepdims=True)


def post_mlp(m0, m1, d0, d1, x, att, g, vec):
    rows = pl.BlockSpec((POST_ROWS, D), lambda i: (i, 0))
    fixed = pl.BlockSpec((8, D), lambda i: (0, 0))
    return pl.pallas_call(
        post_kernel,
        grid=(T // POST_ROWS,),
        in_specs=[rows] * 7 + [fixed],
        out_specs=[rows, rows, rows, fixed],
        out_shape=[jax.ShapeDtypeStruct((T, D), BF16), jax.ShapeDtypeStruct((T, D), F32), jax.ShapeDtypeStruct((T, D), BF16),
                   jax.ShapeDtypeStruct((8, D), F32)],
        compiler_params=pltpu.CompilerParams(dimension_semantics=("arbitrary",)),
        cost_estimate=pl.CostEstimate(flops=5_000_000_000, bytes_accessed=56_000_000, transcendentals=T),
        name="post_mlp",
    )(m0, m1, d0, d1, x, att, g, vec)


def ln_stats(t):
    mean = jnp.mean(t, axis=-1, keepdims=True)
    centered = t - mean
    variance = jnp.mean(centered * centered, axis=-1, keepdims=True)
    rstd = lax.rsqrt(variance + LN_EPS)
    return centered * rstd, rstd


def ln_back(xhat, rstd, d):
    return rstd * (d - jnp.mean(d, axis=-1, keepdims=True) - xhat * jnp.mean(d * xhat, axis=-1, keepdims=True))


LN1_ROWS = 400


def ln1_kernel(d0_ref, d1_ref, w_ref, x_ref, res_ref, vec_ref, dx_ref, sum_ref):
    dh = dot_nt(d0_ref[...], w_ref[:, :3 * HALF]) + dot_nt(d1_ref[...], w_ref[:, 3 * HALF:])
    xhat, rstd = ln_stats(x_ref[...].astype(F32))
    dx_ref[...] = (res_ref[...] + ln_back(xhat, rstd, dh * vec_ref[0:1, :])).astype(BF16)

    @pl.when(pl.program_id(0) == 0)
    def _():
        sum_ref[...] = jnp.zeros_like(sum_ref)

    sum_ref[0:1, :] += jnp.sum(dh * xhat, axis=0, keepdims=True)
    sum_ref[1:2, :] += jnp.sum(dh, axis=0, keepdims=True)


def ln1_backward(d0, d1, w_first, x, res, vec):
    rows = pl.BlockSpec((LN1_ROWS, D), lambda i: (i, 0))
    fixed = pl.BlockSpec((8, D), lambda i: (0, 0))
    return pl.pallas_call(
        ln1_kernel,
        grid=(T // LN1_ROWS,),
        in_specs=[pl.BlockSpec((LN1_ROWS, 3 * HALF), lambda i: (i, 0))] * 2
        + [pl.BlockSpec((D, 3 * D), lambda i: (0, 0), pipeline_mode=pl.Buffered(1)), rows, rows, fixed],
        out_specs=[rows, fixed],
        out_shape=[jax.ShapeDtypeStruct((T, D), BF16), jax.ShapeDtypeStruct((8, D), F32)],
        compiler_params=pltpu.CompilerParams(dimension_semantics=("arbitrary",)),
        cost_estimate=pl.CostEstimate(flops=6 * T * D * D, bytes_accessed=30_000_000, transcendentals=T),
        name="ln1_back",
    )(d0, d1, w_first, x, res, vec)


def gather_rows(shard):
    return lax.all_gather(shard, "fsdp", axis=0, tiled=True)


def exchange(val, bit):
    return lax.ppermute(val, "fsdp", [(i, i ^ bit) for i in range(NS)])


def pick(val, axis, index):
    return lax.dynamic_index_in_dim(val, index, axis, keepdims=False)


class Reduction:
    def __init__(self, send, keep, core, x_first, first=0):
        self.rows, self.cols = send.shape[2:]
        self.keep, self.core, self.x_first, self.first = keep, core, x_first, first
        self.near_bit, self.far_bit = (2, 4) if x_first else (4, 2)
        self.got1 = exchange(send, 1)

    def pick_yx(self, near, far):
        return (far, near) if self.x_first else (near, far)

    def term_specs(self, rows, near, far, at):
        def keep_map(s, idx):
            core = idx[2] if self.core else 0
            return (*self.pick_yx(near(s, idx), far(s, idx)), core, self.first // rows + at(s), 0)

        def got_map(s, idx):
            return (*self.pick_yx(near(s, idx), far(s, idx)), at(s), 0)

        return [(self.keep, pl.BlockSpec((None, None, None, rows, self.cols), keep_map)),
                (self.got1, pl.BlockSpec((None, None, rows, self.cols), got_map))]

    def plan(self, stage, n):
        mine = (lambda idx: idx[0], lambda idx: idx[1]) if self.x_first else (lambda idx: idx[1], lambda idx: idx[0])
        my_near, my_far = mine
        if stage == "near":
            per = n // 2
            rows = self.rows // per
            ins = self.term_specs(rows, lambda s, idx: 1 - my_near(idx), lambda s, idx: s // per, lambda s: s % per)
            return ins, (2, self.rows, self.cols), pl.BlockSpec((None, rows, self.cols), lambda s, idx: (s // per, s % per, 0))
        rows = self.rows // n
        far = (lambda s, idx: 1 - my_far(idx)) if stage == "far" else (lambda s, idx: my_far(idx))
        ins = self.term_specs(rows, lambda s, idx: my_near(idx), far, lambda s: s)
        ins.append((self.got2, pl.BlockSpec((None, rows, self.cols), lambda s, idx: (far(s, idx), s, 0))))
        flat = pl.BlockSpec((rows, self.cols), lambda s, idx: (s, 0))
        if stage == "rep":
            ins.append((self.got3, flat))
        return ins, (self.rows, self.cols), flat

    def start(self, stage, value):
        if stage == "near":
            self.got2 = exchange(value, self.near_bit)
        elif stage == "far":
            self.got3 = exchange(value, self.far_bit)
        else:
            self.part = value
            self.got4 = lax.ppermute(value, "rep", [(0, 1), (1, 0)])

    def result(self):
        return self.part + self.got4


def moves_kernel(counts, idx_ref, *refs):
    outs = refs[sum(counts):]
    at = 0
    for count, out in zip(counts, outs):
        total = refs[at][...]
        for ref in refs[at + 1:at + count]:
            total = total + ref[...]
        out[...] = total
        at += count


MOVE_STEPS = 4


def advance(anchor, *moves):
    flat = [(r, stage) for group, stage in moves for r in group]
    plans = [r.plan(stage, MOVE_STEPS) for r, stage in flat]
    me = lax.axis_index("fsdp")
    idx = jnp.stack([lax.rem(me // 2, 2), me // 4, lax.rem(me, 2)]).astype(jnp.int32)
    values = pl.pallas_call(
        functools.partial(moves_kernel, [len(ins) for ins, _, _ in plans]),
        grid_spec=pltpu.PrefetchScalarGridSpec(
            num_scalar_prefetch=1, grid=(MOVE_STEPS,),
            in_specs=[spec for ins, _, _ in plans for _, spec in ins],
            out_specs=[spec for _, _, spec in plans]),
        out_shape=[jax.ShapeDtypeStruct(shape, F32) for _, shape, _ in plans],
        compiler_params=pltpu.CompilerParams(dimension_semantics=("arbitrary",)),
        cost_estimate=pl.CostEstimate(flops=1_000_000_000, bytes_accessed=10_000_000, transcendentals=0),
        name="moves",
    )(idx, *[val for ins, _, _ in plans for val, _ in ins])
    anchor, values = lax.optimization_barrier((anchor, values))
    for (r, stage), value in zip(flat, values):
        r.start(stage, value)
    return anchor


def split_full(full, pieces):
    rows = full.shape[0] // NS
    parts = full.reshape(2, 2, 2, rows, full.shape[1])
    core = lax.rem(lax.axis_index("fsdp"), 2)
    cut = rows // pieces
    return [Reduction(pick(parts[:, :, :, i * cut:(i + 1) * cut], 2, 1 - core), parts, True, i % 2 == 0, i * cut)
            for i in range(pieces)]


def finish_mlp_kernel(up0, up0_got, up1, up1_got, down0, down0_got, down1, down1_got, up_ref, down_ref):
    up_ref[:, :FC] = up0[...] + up0_got[...]
    up_ref[:, FC:] = up1[...] + up1_got[...]
    down_ref[:FC, :] = (down0[...] + down0_got[...]).T
    down_ref[FC:, :] = (down1[...] + down1_got[...]).T


def finish_mlp(mlp):
    rows = D // NS
    ups = [val for pair in mlp for val in (pair[0].part, pair[0].got4)]
    downs = [val for pair in mlp for val in (pair[1].part, pair[1].got4)]
    return pl.pallas_call(
        finish_mlp_kernel,
        grid=(NS,),
        in_specs=[pl.BlockSpec((rows, FC), lambda s: (0, s))] * 4 + [pl.BlockSpec((rows, FC), lambda s: (s, 0))] * 4,
        out_specs=[pl.BlockSpec((rows, 2 * FC), lambda s: (0, s)), pl.BlockSpec((2 * FC, rows), lambda s: (0, s))],
        out_shape=[jax.ShapeDtypeStruct((rows, FF), F32), jax.ShapeDtypeStruct((FF // NS, D), F32)],
        compiler_params=pltpu.CompilerParams(dimension_semantics=("arbitrary",)),
        cost_estimate=pl.CostEstimate(flops=1_000_000_000, bytes_accessed=12_000_000, transcendentals=0),
        name="finish_mlp",
    )(*ups, *downs)


def finish_attn_kernel(*refs):
    out_ref, qkv_ref = refs[12:]
    cut = D // NS // 2
    for i in range(2):
        rows = slice(i * cut, (i + 1) * cut)
        for half in range(2):
            at = 4 + 4 * half + 2 * i
            qkv_ref[rows, half * HALF:(half + 1) * HALF] = refs[at][...] + refs[at + 1][...]

    @pl.when(pl.program_id(0) == 0)
    def _():
        for i in range(2):
            out_ref[i * cut:(i + 1) * cut, :] = refs[2 * i][...] + refs[2 * i + 1][...]


def finish_attn(out_red, qkv0, qkv1):
    rows = D // NS
    vals = [val for r in (*out_red, *qkv0, *qkv1) for val in (r.part, r.got4)]
    return pl.pallas_call(
        finish_attn_kernel,
        grid=(3,),
        in_specs=[pl.BlockSpec((rows // 2, D), lambda s: (0, 0))] * 4 + [pl.BlockSpec((rows // 2, HALF), lambda s: (0, s))] * 8,
        out_specs=[pl.BlockSpec((rows, D), lambda s: (0, 0)), pl.BlockSpec((rows, D), lambda s: (0, s))],
        out_shape=[jax.ShapeDtypeStruct((rows, D), F32), jax.ShapeDtypeStruct((rows, 3 * D), F32)],
        compiler_params=pltpu.CompilerParams(dimension_semantics=("arbitrary",)),
        cost_estimate=pl.CostEstimate(flops=1_000_000_000, bytes_accessed=6_000_000, transcendentals=0),
        name="finish_attn",
    )(*vals)


def row_major(val):
    return with_layout_constraint(val, Layout(major_to_minor=tuple(range(val.ndim))))


def solution(mesh):
    batch_spec = P(("rep", "fsdp"), None, None)
    row_spec = P("fsdp", None)
    flat_spec = P("fsdp")
    col_spec = P(None, "fsdp")
    param_specs = (row_spec, flat_spec, row_spec, row_spec, flat_spec, row_spec, col_spec)

    def layer_step(x_loc, dz_loc, w_qkv, b_qkv, w_out, w_up, b_up, w_down, vec_params):
        def by_half(val):
            lead = val.shape[:-1]
            return val.reshape(lead + (3, 2, HALF)).swapaxes(-3, -2).reshape(lead + (3 * D,))

        def from_half(val):
            lead = val.shape[:-1]
            return val.reshape(lead + (2, 3, HALF)).swapaxes(-3, -2).reshape(lead + (3 * D,))

        w_first = row_major(jnp.concatenate([by_half(w_qkv.astype(BF16)), w_out.astype(BF16)], axis=1))
        w_first = row_major(gather_rows(w_first))
        wq = w_first[:, :3 * D]
        wo = w_first[:, 3 * D:]
        up_split = w_up.reshape(D // NS, NS, CHUNKS, FC)
        down_split = w_down.reshape(CHUNKS, 2, D // NS, D)
        w_mlp = []
        for c in range(CHUNKS):
            up = up_split[:, :, c].reshape(D // NS, NS * FC).astype(BF16)
            down = jnp.concatenate([down_split[c, 0], down_split[c, 1]], axis=1).astype(BF16)
            shard = row_major(jnp.concatenate([up, down], axis=0))
            w_mlp.append(row_major(lax.all_gather(shard, "fsdp", axis=0, tiled=False)))
        small = jnp.concatenate([b_qkv, b_up, vec_params.reshape(-1)]).astype(BF16)
        small = lax.all_gather(small, "fsdp", axis=0, tiled=False).astype(F32)
        nq, nu = b_qkv.shape[0], b_up.shape[0]
        bias_qkv = by_half(small[:, :nq].reshape(-1))
        bias_up = small[:, nq:nq + nu].reshape(NS, CHUNKS, FC)
        vec = small[:, nq + nu:].reshape(NS, 8, D // NS).transpose(1, 0, 2).reshape(8, D)
        ln1_gain, ln1_bias, out_bias, scale_attn, ln2_gain, ln2_bias, _, scale_mlp = vec

        x_flat = row_major(x_loc.reshape(T, D))
        g_flat = row_major(dz_loc.reshape(T, D))
        x = x_flat.astype(F32)
        d_mlp_bf = row_major((g_flat.astype(F32) * scale_mlp).astype(BF16))
        d_mlp_t = d_mlp_bf.T

        xhat1, _ = ln_stats(x)
        h1 = (xhat1 * ln1_gain + ln1_bias).astype(BF16)
        qkv = (dot(h1, wq) + bias_qkv).astype(BF16)
        heads = attn_forward(qkv)
        att = dot(heads, wo) + out_bias
        y = x + scale_attn * att
        xhat2, _ = ln_stats(y)
        h2 = row_major((xhat2 * ln2_gain + ln2_bias).astype(BF16))
        h2_t = h2.T

        quad = lambda v: v.reshape((2, 2) + v.shape[1:])
        five = lambda v: v.reshape((2, 2, 1) + v.shape[1:])
        partial = []
        grad_bup = []
        mlp = []
        for c in range(CHUNKS):
            m_c, dh_c, up_send, up_keep, down_send, down_keep, gb = mlp_chunk(
                h2, d_mlp_bf, h2_t, d_mlp_t, w_mlp[c], bias_up[:, c].reshape(1, -1))
            mlp.append([Reduction(quad(up_send), five(up_keep), False, True),
                        Reduction(quad(down_send), five(down_keep), False, False)])
            grad_bup.append(gb.reshape(NS, FC))
            partial += [m_c, dh_c]
        partial = advance(partial, (mlp[0], "near"))
        z, g_resid, d_att_bf, vec_sums = post_mlp(partial[0], partial[2], partial[1], partial[3], x_flat, att, g_flat, vec)
        z = row_major(z.reshape(SEQS, SEQ, D))
        d_heads = dot_nt(d_att_bf, wo).astype(BF16)
        out_red = split_full(dot_tn(heads, d_att_bf), 2)

        d_heads = advance(d_heads, (mlp[0], "far"), (mlp[1], "near"))
        d_qkv0, gb0 = attn_backward(qkv, d_heads, 0)
        qkv0 = split_full(dot_tn(h1, d_qkv0), 2)
        d_heads = advance(d_heads, (out_red, "near"), (mlp[0], "rep"))
        d_heads = advance(d_heads, (mlp[1], "far"), (qkv0, "near"))
        d_qkv1, gb1 = attn_backward(qkv, d_heads, 1)
        gw1 = dot_tn(h1, d_qkv1)
        qkv1 = split_full(gw1, 2)
        d_qkv1 = advance(d_qkv1, (qkv0, "far"), (out_red, "far"), (mlp[1], "rep"))
        d_qkv1 = advance(d_qkv1, (qkv1, "near"))
        dx, ln1_sums = ln1_backward(d_qkv0, d_qkv1, w_first, x_flat, g_resid, vec)
        done = [(r.part, r.got4) for r in mlp[0]]
        dx, z, done = lax.optimization_barrier((dx, z, done))
        for r, (r.part, r.got4) in zip(mlp[0], done):
            pass
        grad_vec = jnp.concatenate([ln1_sums[:2], vec_sums[2:]], axis=0)
        grad_bqkv = from_half(jnp.sum(jnp.concatenate([gb0, gb1], axis=2), axis=(0, 1))).reshape(NS, nq)
        grad_bup = jnp.stack(grad_bup, axis=1).reshape(NS, nu)
        grad_vec = grad_vec.reshape(8, NS, D // NS).transpose(1, 0, 2).reshape(NS, D)
        small_grads = jnp.concatenate([grad_bqkv, grad_bup, grad_vec, jnp.zeros((NS, 64 * 128 - nq - nu - D), F32)], axis=1)
        small_red = split_full(small_grads.reshape(NS * 64, 128), 1)
        dx = advance(dx, (qkv1, "far"), (out_red, "rep"), (qkv0, "rep"))
        dx = row_major(dx.reshape(SEQS, SEQ, D))
        advance((), (qkv1, "rep"), (small_red, "near"))
        advance((), (small_red, "far"))
        advance((), (small_red, "rep"))
        grad_up, grad_down = finish_mlp(mlp)
        grad_w_out, grad_w_qkv = finish_attn(out_red, qkv0, qkv1)
        mine = small_red[0].result().reshape(-1)
        return (z, dx, grad_w_qkv, mine[:nq], grad_w_out, grad_up, mine[nq:nq + nu], grad_down,
                mine[nq + nu:nq + nu + D].reshape(8, D // NS))

    return jax.shard_map(layer_step, mesh=mesh, in_specs=(batch_spec, batch_spec) + param_specs,
                         out_specs=(batch_spec, batch_spec) + param_specs, check_vma=False)
```
